256 devices in a mesh: groups: 4 (over y, x), pb: 64 (over z, core).
Axes of the slice: x: 2, y: 2, z: 32, core: 2. Of those that a mesh axis runs over, the one named last changes fastest.
The devices are a block of a 4x8x32 slice.
Arguments:
- eigvec: bfloat16 [65536, 2592], P(('groups', 'pb')), parts along dimension 0, may hold values from -0.69921875 to 0.69921875
- omega: bfloat16 [65536, 36], P(('groups', 'pb')), parts along dimension 0, may hold values from 0.5 to 4
- phi: bfloat16 [36, 36, 36], replicated, may hold values from -6 to 6
- send_rows: int32 [256, 128], P(('groups', 'pb')), parts along dimension 0, may hold values from 0 to 255
- local_q: int32 [4096], P(('groups', 'pb')), parts along dimension 0, may hold values from 0 to 255
- partner_q: int32 [4096], P(('groups', 'pb')), parts along dimension 0, may hold values from 0 to 255
- slot_ref: int32 [4096], P(('groups', 'pb')), parts along dimension 0, may hold values from 0 to 127, as said below
- tri_count: int32 [256], P(('groups', 'pb')), parts along dimension 0, may hold values from 8 to 16, as said below
Outputs:
- rates: float32 [36, 65536], P(None, ('groups', 'pb')), parts along dimension 1
The draws below stay inside these ranges and needn't reach their ends.
There are 4 independent parts, one for each index of `groups`. The reference program is written for one: setup_inputs(seed, part) draws one part's arguments, and reference() takes and returns one part's arrays. A program takes and returns all parts, laid end to end along the dimension named above; an argument that names none is the same for every part. Nothing has to cross between parts.
Inputs may be any that keep to these rules, and one draw needn't show every extreme that they name: slot_ref of a live triplet of device p names an owner o and a slot s below the number of slots that o fills for p, which is 1 to 2; each device receives 2 filled slots from some owner. `tri_count`: exactly one device has 16 live triplets; live triplets come first.
All inputs are finite; a program needn't handle non-finite values.
Results may differ from the reference program's by a relative error of at most 0.00048.
Values may be sent and summed in bfloat16 or wider, within the bound.
A program may use at most 128 MiB of HBM per device.

```python
import jax
import jax.numpy as jnp
from jax import lax

NB = 36
QDEV = 256
CAP = 2
TRI_CAP = 16
Q = 16384
TRIPLETS = 1024
N_PB = 64


def draw_omega(key, part):
    freq_key = jax.random.fold_in(key, 31)
    logs = jax.random.uniform(freq_key, (QDEV * N_PB, NB), jnp.float32, jnp.log(0.5), jnp.log(4.0))
    values = jnp.clip(jnp.exp(logs), 0.5, 4.0)
    return values.astype(jnp.bfloat16)


def draw_slot_ref(key, part):
    count_key = jax.random.fold_in(key, 11)
    owner_key = jax.random.fold_in(key, 12)
    slot_key = jax.random.fold_in(key, 13)
    filled = jax.random.randint(count_key, (N_PB, N_PB), 1, CAP + 1)
    dest = jnp.arange(N_PB, dtype=jnp.int32)
    full_owner = (dest + 1) % N_PB
    filled = filled.at[full_owner, dest].set(CAP)
    device = jnp.arange(TRI_CAP * N_PB, dtype=jnp.int32) // TRI_CAP
    owner = jax.random.randint(owner_key, (TRI_CAP * N_PB,), 0, N_PB)
    limit = filled[owner, device]
    slot = jax.random.randint(slot_key, (TRI_CAP * N_PB,), 0, CAP) % limit
    return (owner * CAP + slot).astype(jnp.int32)


def draw_tri_count(key, part):
    count_key = jax.random.fold_in(key, 21)
    pick_key = jax.random.fold_in(key, 22)
    lowest = max(1, TRI_CAP // 2)
    counts = jax.random.randint(count_key, (N_PB,), lowest, TRI_CAP)
    busiest = jax.random.randint(pick_key, (), 0, N_PB)
    counts = counts.at[busiest].set(TRI_CAP)
    return counts.astype(jnp.int32)


def touch_ends(entries, rng, low, top_value):
    shape = entries.shape
    index_at = [jax.random.randint(jax.random.fold_in(rng, axis), (), 0, shape[axis]) for axis in range(len(shape))]
    entries = entries.at[tuple(index_at)].set(low)
    longest = shape.index(max(shape))
    index_at[longest] = (index_at[longest] + 1) % shape[longest]
    return entries.at[tuple(index_at)].set(top_value)


def block_levels(stream_key, shape, pieces, smallest, largest):
    def one(dim, shards_of):
        draws = jax.random.uniform(jax.random.fold_in(jax.random.fold_in(stream_key, 6), dim), (shards_of,), jnp.float32, smallest / len(pieces), largest / len(pieces))
        return jnp.repeat(jnp.exp(draws), shape[dim] // shards_of).reshape((-1,) + (1,) * (len(shape) - dim - 1))

    factor_of = one(*pieces[0])
    for cut in pieces[1:]:
        factor_of = factor_of * one(*cut)
    return factor_of


def centred(stream_key, shape, width, most, cuts=(), held_as=jnp.bfloat16):
    array = width * jax.random.normal(stream_key, shape, jnp.float32)
    if cuts:
        array = array * block_levels(stream_key, shape, cuts, -0.22, 0.18)
    return jnp.clip(array, -most, most).astype(held_as)


def setup_inputs(seed: int = 0, part: int = 0) -> dict:
    keys = jax.random.split(jax.random.key(seed), 9)
    own_keys = jax.random.split(jax.random.fold_in(keys[8], part), 9)
    return {
        "eigvec": centred(own_keys[0], (Q, 2 * NB * NB), 0.118, 0.69921875, ((0, 64),)),
        "omega": draw_omega(jax.random.fold_in(jax.random.fold_in(keys[8], part), 71), part),
        "phi": centred(keys[2], (NB, NB, NB), 1.0, 6.0),
        "send_rows": touch_ends(jax.random.randint(own_keys[3], (N_PB, N_PB * CAP), 0, QDEV), jax.random.fold_in(own_keys[3], 1), 0, QDEV - 1).astype(jnp.int32),
        "local_q": touch_ends(jax.random.randint(own_keys[4], (TRIPLETS,), 0, QDEV), jax.random.fold_in(own_keys[4], 1), 0, QDEV - 1).astype(jnp.int32),
        "partner_q": touch_ends(jax.random.randint(own_keys[5], (TRIPLETS,), 0, QDEV), jax.random.fold_in(own_keys[5], 1), 0, QDEV - 1).astype(jnp.int32),
        "slot_ref": draw_slot_ref(jax.random.fold_in(jax.random.fold_in(keys[8], part), 71), part),
        "tri_count": draw_tri_count(jax.random.fold_in(jax.random.fold_in(keys[8], part), 71), part),
    }


smear_width = 0.5


def triplet_rates(phi, near_vec, partner_vec, far_vec, near_freq, partner_freq, far_freq, weight_mask):
    phi_full = phi.astype(jnp.float32)
    far_real = far_vec[:, 0].astype(jnp.float32)
    far_imag = far_vec[:, 1].astype(jnp.float32)
    y_real = jnp.einsum('abc,tnc->tabn', phi_full, far_real)
    y_imag = -jnp.einsum('abc,tnc->tabn', phi_full, far_imag)
    y_real = y_real.astype(jnp.bfloat16).astype(jnp.float32)
    y_imag = y_imag.astype(jnp.bfloat16).astype(jnp.float32)
    part_real = partner_vec[:, 0].astype(jnp.float32)
    part_imag = partner_vec[:, 1].astype(jnp.float32)
    z_real = jnp.einsum('tmb,tabn->tamn', part_real, y_real) - jnp.einsum('tmb,tabn->tamn', part_imag, y_imag)
    z_imag = jnp.einsum('tmb,tabn->tamn', part_real, y_imag) + jnp.einsum('tmb,tabn->tamn', part_imag, y_real)
    z_real = z_real.astype(jnp.bfloat16).astype(jnp.float32)
    z_imag = z_imag.astype(jnp.bfloat16).astype(jnp.float32)
    near_real = near_vec[:, 0].astype(jnp.float32)
    near_imag = near_vec[:, 1].astype(jnp.float32)
    v_real = jnp.einsum('tva,tamn->tvmn', near_real, z_real) - jnp.einsum('tva,tamn->tvmn', near_imag, z_imag)
    v_imag = jnp.einsum('tva,tamn->tvmn', near_real, z_imag) + jnp.einsum('tva,tamn->tvmn', near_imag, z_real)
    power = v_real * v_real + v_imag * v_imag
    first = near_freq.astype(jnp.float32)[:, :, None, None]
    second = partner_freq.astype(jnp.float32)[:, None, :, None]
    third = far_freq.astype(jnp.float32)[:, None, None, :]
    offset = (first + second - third) / smear_width
    weight = jnp.exp(-offset * offset) / (first * second * third * NB)
    terms = power * weight * weight_mask[:, None, None, None]
    return jnp.sum(terms, axis=(2, 3)), jnp.sum(terms, axis=(1, 2))


def reference(eigvec, omega, phi, send_rows, local_q, partner_q, slot_ref, tri_count):
    total_q = QDEV * N_PB
    slot_index = jnp.arange(TRI_CAP * N_PB, dtype=jnp.int32)
    device = slot_index // TRI_CAP
    within = slot_index % TRI_CAP
    weight_mask = (within < tri_count[device]).astype(jnp.float32)
    owner = slot_ref // CAP
    column = device * CAP + slot_ref % CAP
    far_global = owner * QDEV + send_rows[owner, column]
    near_global = device * QDEV + local_q
    partner_global = device * QDEV + partner_q

    def one_device(packed):
        near_idx, partner_idx, far_idx, mask_part = packed
        near_vec = eigvec[near_idx].reshape(TRI_CAP, 2, NB, NB)
        partner_vec = eigvec[partner_idx].reshape(TRI_CAP, 2, NB, NB)
        far_vec = eigvec[far_idx].reshape(TRI_CAP, 2, NB, NB)
        return triplet_rates(phi, near_vec, partner_vec, far_vec, omega[near_idx], omega[partner_idx], omega[far_idx], mask_part)

    near_terms, far_terms = lax.map(one_device, (near_global.reshape(N_PB, TRI_CAP), partner_global.reshape(N_PB, TRI_CAP), far_global.reshape(N_PB, TRI_CAP), weight_mask.reshape(N_PB, TRI_CAP)))
    near_terms = near_terms.reshape(TRI_CAP * N_PB, NB)
    far_terms = far_terms.reshape(TRI_CAP * N_PB, NB)
    rates = jnp.zeros((NB, total_q), jnp.float32)
    rates = rates.at[:, near_global].add(near_terms.T)
    rates = rates.at[:, far_global].add(far_terms.T)
    return rates
```

```python
import functools
import math

import jax
import jax.numpy as jnp
from jax import lax
from jax.experimental import pallas as pl
from jax.experimental.pallas import tpu as pltpu
from jax.sharding import PartitionSpec as P

LANES = 128
IM = 64
KP = 40
smear_width = 0.5
MESH = pl.DeviceIdType.MESH


def lane_iota(shape):
    return lax.broadcasted_iota(jnp.int32, shape, len(shape) - 1)


def shifted_window(tiles, start, width, to):
    first, at = divmod(start, LANES)
    moved = pltpu.roll(tiles(first), (to - at) % LANES, 1) if to != at else tiles(first)
    if at + width > LANES:
        after = pltpu.roll(tiles(first + 1), (to - at) % LANES, 1)
        moved = jnp.where(lane_iota(moved.shape) < to + LANES - at, moved, after)
    return moved


def spread_rows(tiles, nb, out_ref, im_at, both):
    half = nb * nb

    def put(k, value):
        count = value.shape[0]
        out_ref[k * count : (k + 1) * count, :] = value

    for k in range(nb):
        re = shifted_window(tiles, k * nb, nb, 0)
        im = shifted_window(tiles, half + k * nb, nb, im_at)
        lanes = lane_iota(re.shape)
        in_re = lanes < nb
        in_im = (lanes >= im_at) & (lanes < im_at + nb)
        put(k, jnp.where(in_re, re, jnp.where(in_im, im, 0.0)))
        if both:
            im0 = shifted_window(tiles, half + k * nb, nb, 0)
            re1 = shifted_window(tiles, k * nb, nb, im_at)
            put(KP + k, jnp.where(in_re, -im0, jnp.where(in_im, re1, 0.0)))
    zero = jnp.zeros(re.shape, jnp.float32)
    for k in range(nb, KP):
        put(k, zero)
        if both:
            put(KP + k, zero)


def picked(index_row, count):
    width = index_row.shape[1]
    hot = lax.broadcasted_iota(jnp.int32, (count, width), 0) == index_row
    return hot.astype(jnp.float32)


def rate_kernel(
    n,
    nb,
    slots,
    send_ref,
    near_ref,
    part_ref,
    phi_ref,
    rows_ref,
    local_ref,
    slot_ref,
    slot_s,
    live_s,
    out_ref,
    recv,
    mat,
    near_mat,
    far_mat,
    far_rows,
    inner,
    outer,
    second,
    near_acc,
    far_acc,
    by_slot,
    returned,
    send_sem,
    recv_sem,
    back_send,
    back_recv,
):
    me = lax.axis_index("pb")
    trip = near_ref.shape[0]
    width = send_ref.shape[2]
    freq_at = 2 * nb * nb
    quads = nb // 4

    def peer(i):
        off = (i + 1) // 2
        step = n // 2 + jnp.where(i % 2 == 0, off, -off)
        return step, lax.rem(me + step, n)

    def exchange(i):
        step, to = peer(i)
        return pltpu.make_async_remote_copy(
            src_ref=send_ref.at[to],
            dst_ref=recv.at[me],
            send_sem=send_sem.at[step],
            recv_sem=recv_sem.at[step],
            device_id={"pb": to},
            device_id_type=MESH,
        )

    def give_back(i):
        step, to = peer(i)
        return pltpu.make_async_remote_copy(
            src_ref=by_slot.at[to],
            dst_ref=returned.at[me],
            send_sem=back_send.at[step],
            recv_sem=back_recv.at[step],
            device_id={"pb": to},
            device_id_type=MESH,
        )

    barrier = pltpu.get_barrier_semaphore()

    def greet(i, carry):
        _, to = peer(i)
        pl.semaphore_signal(barrier, inc=1, device_id={"pb": to}, device_id_type=MESH)
        return carry

    lax.fori_loop(0, n - 1, greet, 0)
    pl.semaphore_wait(barrier, n - 1)

    def begin(i, carry):
        exchange(i).start()
        return carry

    lax.fori_loop(0, n - 1, begin, 0)

    def tiles_of(ref):
        return lambda k: ref[:, k * LANES : (k + 1) * LANES].astype(jnp.float32)

    near_tiles, part_tiles = tiles_of(near_ref), tiles_of(part_ref)
    spread_rows(part_tiles, nb, mat, IM, True)
    spread_rows(near_tiles, nb, near_mat, KP, False)

    rows = nb * trip
    pitch = inner.shape[0] // (2 * KP)
    zero_rows = jnp.zeros(((KP - nb) * pitch, LANES), jnp.float32)
    inner[nb * pitch : KP * pitch, :] = zero_rows
    inner[(KP + nb) * pitch : 2 * KP * pitch, :] = zero_rows
    part_re = mat[0:rows, :].astype(jnp.bfloat16)
    part_im = mat[KP * trip : KP * trip + rows, :].astype(jnp.bfloat16)

    def contract_b(a, carry):
        block = phi_ref[a].astype(jnp.float32)
        block = jnp.concatenate([block, jnp.zeros((nb, LANES - nb), jnp.float32)], axis=1)
        block = jnp.concatenate([block, jnp.zeros((KP - nb, LANES), jnp.float32)], axis=0)
        gap = jnp.zeros((IM - KP, LANES), jnp.float32)
        block = jnp.concatenate([block, gap, pltpu.roll(block, IM, 1), gap], axis=0)
        block = block.astype(jnp.bfloat16)
        for part, first in ((part_re, 0), (part_im, KP)):
            at = pl.multiple_of((first + a) * pitch, 8)
            inner[pl.ds(at, rows), :] = jnp.dot(
                part, block, preferred_element_type=jnp.float32
            )
        return carry

    lax.fori_loop(0, nb, contract_b, 0)

    def contract_a(t, carry):
        left = near_mat[pl.ds(t, KP, stride=trip), :]
        left = left[:, 0 : 2 * KP].astype(jnp.bfloat16)
        for quad in range(quads):
            halves = []
            for pair in range(2):
                sides = []
                for one in range(2):
                    m = quad * 4 + pair * 2 + one
                    sides.append(
                        inner[pl.ds(m * trip + t, 2 * KP, stride=pitch), :].astype(
                            jnp.bfloat16
                        )
                    )
                right = jnp.concatenate(sides, axis=1)
                halves.append(jnp.dot(left, right, preferred_element_type=jnp.float32))
            outer[t, quad * 2 * KP : (quad + 1) * 2 * KP, :] = jnp.concatenate(
                halves, axis=0
            ).astype(jnp.bfloat16)
        return carry

    lax.fori_loop(0, trip, contract_a, 0)

    low = freq_at // LANES * LANES
    at = freq_at - low
    part_freq = pltpu.roll(part_tiles(low // LANES), LANES - at, 1)
    near_freq = pltpu.roll(near_tiles(low // LANES), LANES - at, 1)
    second[...] = jnp.where(lane_iota(part_freq.shape) < nb, part_freq, 1.0)
    near_col = jnp.transpose(
        jnp.concatenate([near_freq, jnp.ones((LANES - trip, LANES), jnp.float32)], axis=0)
    )[0:KP]

    recv[me] = send_ref[me]

    def arrived(i, carry):
        copy = exchange(i)
        copy.wait_send()
        copy.wait_recv()
        return carry

    lax.fori_loop(0, n - 1, arrived, 0)

    for t in range(trip):
        where = slot_s[t]
        pair = recv[where // slots].astype(jnp.float32)
        row = pair[0:1]
        for s in range(1, slots):
            row = jnp.where(where % slots == s, pair[s : s + 1], row)
        far_rows[t : t + 1, :] = row

    far_tiles = tiles_of(far_rows)
    spread_rows(far_tiles, nb, far_mat, IM, True)
    far_freq = pltpu.roll(far_tiles(low // LANES), LANES - at, 1)
    lanes = lane_iota(far_freq.shape)
    far_freq = jnp.where(
        lanes < KP,
        far_freq,
        pltpu.roll(far_freq, KP, 1),
    )
    used = (lanes < nb) | ((lanes >= KP) & (lanes < KP + nb))
    far_freq = jnp.where(used, far_freq, 1.0)
    used_row = used[0:1]
    used_cell = (lax.broadcasted_iota(jnp.int32, (KP, LANES), 0) < nb) & (
        jnp.broadcast_to(used_row.astype(jnp.int32), (KP, LANES)) > 0
    )
    scale = math.sqrt(math.log2(math.e)) / smear_width
    live = live_s[0]

    for t in range(trip):
        ef = far_mat[pl.ds(t, 2 * KP, stride=trip), :]
        zero = jnp.zeros((2 * KP, LANES), jnp.float32)
        gap = jnp.zeros((LANES - 2 * KP, 2 * LANES), jnp.float32)
        ef = jnp.concatenate(
            [
                jnp.concatenate([ef, zero], axis=1),
                gap,
                jnp.concatenate([zero, ef], axis=1),
                gap,
            ],
            axis=0,
        ).astype(jnp.bfloat16)
        w1 = jnp.broadcast_to(near_col[:, t : t + 1], (KP, LANES))
        w3 = jnp.broadcast_to(far_freq[t : t + 1, :], (KP, LANES))
        base = (w1 - w3) * scale
        total = jnp.zeros((KP, LANES), jnp.float32)
        v = lax.dot_general(
            outer[t], ef, (((1,), (1,)), ((), ())), preferred_element_type=jnp.float32
        )
        for m in range(nb):
            w2 = jnp.broadcast_to(second[t : t + 1, m : m + 1], (KP, LANES))
            one = v[m // 2 * KP : (m // 2 + 1) * KP, (m % 2) * LANES : (m % 2 + 1) * LANES]
            x = base + w2 * scale
            total = total + one * one * (jnp.exp2(-(x * x)) / w2)
        keep = used_cell & (t < live)
        total = jnp.where(keep, total / (w1 * w3 * nb), 0.0)
        near_sum = jnp.sum(total, axis=1, keepdims=True)
        near_acc[t] = jnp.broadcast_to(near_sum, (KP, LANES))
        far_sum = jnp.sum(total, axis=0, keepdims=True)
        far_sum = far_sum + pltpu.roll(far_sum, LANES - KP, 1)
        far_acc[t : t + 1, :] = jnp.where(lane_iota(far_sum.shape) < nb, far_sum, 0.0)

    spots = lax.broadcasted_iota(jnp.int32, (n, LANES), 0)
    back = jnp.zeros((n, LANES), jnp.float32)
    for t in range(trip):
        where = slot_s[t]
        row = far_acc[t : t + 1, :]
        for s in range(1, slots):
            row = jnp.where(where % slots == s, pltpu.roll(row, s * LANES // slots, 1), row)
        back = back + jnp.where(spots == where // slots, row, 0.0)
    by_slot[...] = back.reshape(n, 1, LANES)
    returned[me] = by_slot[me]

    def begin_back(i, carry):
        give_back(i).start()
        return carry

    lax.fori_loop(0, n - 1, begin_back, 0)

    owned = out_ref.shape[1]
    columns = lane_iota((1, owned))
    rates = jnp.zeros((KP, owned), jnp.float32)
    for t in range(trip):
        spread = jnp.concatenate([near_acc[t]] * (owned // LANES), axis=1)
        rates = rates + jnp.where(columns == local_ref[0:1, t : t + 1], spread, 0.0)

    def arrived_back(i, carry):
        copy = give_back(i)
        copy.wait_send()
        copy.wait_recv()
        return carry

    lax.fori_loop(0, n - 1, arrived_back, 0)

    filled = returned[...].reshape(n, LANES)
    filled_t = jnp.transpose(jnp.concatenate([filled] * (LANES // n), axis=0))
    step = LANES // slots
    for s in range(slots):
        hot = (
            lax.broadcasted_iota(jnp.int32, (owned, LANES), 0) == rows_ref[s : s + 1, :]
        ).astype(jnp.float32)
        rates = rates + lax.dot_general(
            filled_t[s * step : s * step + KP],
            hot,
            (((1,), (1,)), ((), ())),
            precision=lax.Precision.HIGHEST,
            preferred_element_type=jnp.float32,
        )
    out_ref[...] = rates[0:nb]


def on_device(n, eigvec, omega, phi, send_rows, local_q, partner_q, slot_ref, tri_count):
    owned = eigvec.shape[0]
    nb = omega.shape[1]
    trip = local_q.shape[0]
    outgoing = send_rows[0]
    slots = outgoing.shape[0] // n
    width = -(-(eigvec.shape[1] + nb) // LANES) * LANES

    table = jnp.concatenate(
        [
            eigvec,
            omega,
            jnp.zeros((owned, width - eigvec.shape[1] - nb), eigvec.dtype),
        ],
        axis=1,
    )

    def rows_of(index):
        return jnp.take(table, index, axis=0, mode="clip")

    send = rows_of(outgoing).reshape(n, slots, width)
    near, part = rows_of(local_q), rows_of(partner_q)
    places = outgoing.reshape(n, slots).T
    places = jnp.concatenate(
        [places, jnp.full((slots, LANES - n), -1, jnp.int32)], axis=1
    )
    vmem = pl.BlockSpec(memory_space=pltpu.VMEM)
    smem = pl.BlockSpec(memory_space=pltpu.SMEM)
    f32 = jnp.float32
    return pl.pallas_call(
        functools.partial(rate_kernel, n, nb, slots),
        out_shape=jax.ShapeDtypeStruct((nb, owned), f32),
        in_specs=[vmem] * 7 + [smem] * 2,
        out_specs=vmem,
        scratch_shapes=[
            pltpu.VMEM((n, slots, width), jnp.bfloat16),
            pltpu.VMEM((2 * KP * trip, LANES), f32),
            pltpu.VMEM((KP * trip, LANES), f32),
            pltpu.VMEM((2 * KP * trip, LANES), f32),
            pltpu.VMEM((trip, width), f32),
            pltpu.VMEM((2 * KP * (nb * trip + 8), LANES), f32),
            pltpu.VMEM((trip, nb // 2 * KP, 2 * LANES), jnp.bfloat16),
            pltpu.VMEM((trip, LANES), f32),
            pltpu.VMEM((trip, KP, LANES), f32),
            pltpu.VMEM((trip, LANES), f32),
            pltpu.VMEM((n, 1, LANES), f32),
            pltpu.VMEM((n, 1, LANES), f32),
            pltpu.SemaphoreType.DMA((n,)),
            pltpu.SemaphoreType.DMA((n,)),
            pltpu.SemaphoreType.DMA((n,)),
            pltpu.SemaphoreType.DMA((n,)),
        ],
        compiler_params=pltpu.CompilerParams(
            collective_id=0, has_side_effects=True, vmem_limit_bytes=60 * 1024 * 1024
        ),
    )(
        send,
        near,
        part,
        phi,
        places,
        local_q.reshape(1, trip),
        slot_ref.reshape(1, trip),
        slot_ref,
        tri_count,
    )


def solution(mesh):
    in_specs = (
        P(("groups", "pb"), None),
        P(("groups", "pb"), None),
        P(),
        P(("groups", "pb"), None),
        P(("groups", "pb")),
        P(("groups", "pb")),
        P(("groups", "pb")),
        P(("groups", "pb")),
    )
    out_specs = P(None, ("groups", "pb"))
    return jax.shard_map(
        functools.partial(on_device, mesh.shape["pb"]),
        mesh=mesh,
        in_specs=in_specs,
        out_specs=out_specs,
        check_vma=False,
    )
```

```python
import functools
import math

import jax
import jax.numpy as jnp
from jax import lax
from jax.experimental import pallas as pl
from jax.experimental.pallas import tpu as pltpu
from jax.sharding import PartitionSpec as P

LANES = 128
IM = 64
KP = 40
smear_width = 0.5
MESH = pl.DeviceIdType.MESH


def lane_iota(shape):
    return lax.broadcasted_iota(jnp.int32, shape, len(shape) - 1)


def shifted_window(tiles, start, width, to):
    first, at = divmod(start, LANES)
    moved = pltpu.roll(tiles(first), (to - at) % LANES, 1) if to != at else tiles(first)
    if at + width > LANES:
        after = pltpu.roll(tiles(first + 1), (to - at) % LANES, 1)
        moved = jnp.where(lane_iota(moved.shape) < to + LANES - at, moved, after)
    return moved


def spread_rows(tiles, nb, out_ref, im_at, both):
    half = nb * nb

    def put(k, value):
        count = value.shape[0]
        out_ref[k * count : (k + 1) * count, :] = value

    for k in range(nb):
        re = shifted_window(tiles, k * nb, nb, 0)
        im = shifted_window(tiles, half + k * nb, nb, im_at)
        lanes = lane_iota(re.shape)
        in_re = lanes < nb
        in_im = (lanes >= im_at) & (lanes < im_at + nb)
        put(k, jnp.where(in_re, re, jnp.where(in_im, im, 0.0)))
        if both:
            im0 = shifted_window(tiles, half + k * nb, nb, 0)
            re1 = shifted_window(tiles, k * nb, nb, im_at)
            put(KP + k, jnp.where(in_re, -im0, jnp.where(in_im, re1, 0.0)))
    zero = jnp.zeros(re.shape, jnp.float32)
    for k in range(nb, KP):
        put(k, zero)
        if both:
            put(KP + k, zero)


def picked(index_row, count):
    width = index_row.shape[1]
    hot = lax.broadcasted_iota(jnp.int32, (count, width), 0) == index_row
    return hot.astype(jnp.float32)


def rate_kernel(
    n,
    nb,
    slots,
    eig_hbm,
    omega_ref,
    phi_hbm,
    rows_ref,
    local_ref,
    partner_ref,
    slot_s,
    live_s,
    out_ref,
    eig_ref,
    phi_ref,
    send_ref,
    near_ref,
    part_ref,
    places,
    recv,
    mat,
    near_mat,
    far_mat,
    far_rows,
    inner,
    outer,
    second,
    third,
    near_acc,
    far_acc,
    by_slot,
    returned,
    send_sem,
    recv_sem,
    back_send,
    back_recv,
    load_sem,
):
    me = lax.axis_index("pb")
    trip = near_ref.shape[0]
    owned = out_ref.shape[1]
    freq_at = 2 * nb * nb
    quads = nb // 4

    def peer(i):
        off = (i + 1) // 2
        step = n // 2 + jnp.where(i % 2 == 0, off, -off)
        return lax.rem(me + step, n)

    def all_moved(ref, sem):
        every = ref.at[pl.ds(0, n - 1)]
        pltpu.make_async_copy(every, every, sem.at[0]).wait()

    def exchange(i):
        to = peer(i)
        return pltpu.make_async_remote_copy(
            src_ref=send_ref.at[to],
            dst_ref=recv.at[me],
            send_sem=send_sem.at[0],
            recv_sem=recv_sem.at[0],
            device_id={"pb": to},
            device_id_type=MESH,
        )

    def give_back(i):
        to = peer(i)
        return pltpu.make_async_remote_copy(
            src_ref=by_slot.at[to],
            dst_ref=returned.at[me],
            send_sem=back_send.at[0],
            recv_sem=back_recv.at[0],
            device_id={"pb": to},
            device_id_type=MESH,
        )

    load_eig = pltpu.make_async_copy(eig_hbm, eig_ref, load_sem.at[0])
    load_phi = pltpu.make_async_copy(phi_hbm, phi_ref, load_sem.at[1])
    load_eig.start()
    load_phi.start()
    barrier = pltpu.get_barrier_semaphore()

    def greet(i, carry):
        to = peer(i)
        pl.semaphore_signal(barrier, inc=1, device_id={"pb": to}, device_id_type=MESH)
        return carry

    lax.fori_loop(0, n - 1, greet, 0)

    rest = jnp.full((1, LANES - 2 * trip), -1, jnp.int32)
    own_row = jnp.concatenate([local_ref[...], partner_ref[...], rest], axis=1)
    hot_send = jnp.transpose(picked(rows_ref[...], owned)).astype(jnp.bfloat16)
    hot_own = jnp.transpose(picked(own_row, owned))[0 : 2 * trip].astype(jnp.bfloat16)
    hot = jnp.concatenate([hot_send, hot_own], axis=0)
    sent = n * slots
    load_eig.wait()
    low = freq_at // LANES * LANES
    tail = jnp.concatenate(
        [
            eig_ref[low:freq_at, :].astype(jnp.float32),
            omega_ref[...].astype(jnp.float32),
            jnp.zeros((low + LANES - freq_at - nb, owned), jnp.float32),
        ],
        axis=0,
    ).astype(jnp.bfloat16)
    piece = 2 * LANES
    for start in range(0, low + LANES, piece):
        end = min(start + piece, low + LANES)
        table = tail if start == low else eig_ref[start:end, :]
        rows = lax.dot_general(
            hot, table, (((1,), (1,)), ((), ())), preferred_element_type=jnp.float32
        )
        send_ref[:, :, start:end] = (
            rows[0:sent].astype(jnp.bfloat16).reshape(n, slots, end - start)
        )
        near_ref[:, start:end] = rows[sent : sent + trip]
        part_ref[:, start:end] = rows[sent + trip : sent + 2 * trip]

    pl.semaphore_wait(barrier, n - 1)

    def begin(i, carry):
        exchange(i).start()
        return carry

    lax.fori_loop(0, n - 1, begin, 0)

    def tiles_of(ref):
        return lambda k: ref[:, k * LANES : (k + 1) * LANES]

    near_tiles, part_tiles = tiles_of(near_ref), tiles_of(part_ref)
    spread_rows(part_tiles, nb, mat, IM, True)
    spread_rows(near_tiles, nb, near_mat, KP, False)

    rows = nb * trip
    pitch = inner.shape[0] // (2 * KP)
    zero_rows = jnp.zeros(((KP - nb) * pitch, LANES), jnp.float32)
    inner[nb * pitch : KP * pitch, :] = zero_rows
    inner[(KP + nb) * pitch : 2 * KP * pitch, :] = zero_rows
    part_re = mat[0:rows, :].astype(jnp.bfloat16)
    part_im = mat[KP * trip : KP * trip + rows, :].astype(jnp.bfloat16)

    def contract_b(a, carry):
        block = phi_ref[a].astype(jnp.float32)
        block = jnp.concatenate([block, jnp.zeros((nb, LANES - nb), jnp.float32)], axis=1)
        block = jnp.concatenate([block, jnp.zeros((KP - nb, LANES), jnp.float32)], axis=0)
        gap = jnp.zeros((IM - KP, LANES), jnp.float32)
        block = jnp.concatenate([block, gap, pltpu.roll(block, IM, 1), gap], axis=0)
        block = block.astype(jnp.bfloat16)
        for part, first in ((part_re, 0), (part_im, KP)):
            at = pl.multiple_of((first + a) * pitch, 8)
            inner[pl.ds(at, rows), :] = jnp.dot(
                part, block, preferred_element_type=jnp.float32
            )
        return carry

    load_phi.wait()
    lax.fori_loop(0, nb, contract_b, 0)

    def contract_a(t, carry):
        left = near_mat[pl.ds(t, KP, stride=trip), :]
        left = left[:, 0 : 2 * KP].astype(jnp.bfloat16)
        for quad in range(quads):
            halves = []
            for pair in range(2):
                sides = []
                for one in range(2):
                    m = quad * 4 + pair * 2 + one
                    sides.append(
                        inner[pl.ds(m * trip + t, 2 * KP, stride=pitch), :].astype(
                            jnp.bfloat16
                        )
                    )
                right = jnp.concatenate(sides, axis=1)
                halves.append(jnp.dot(left, right, preferred_element_type=jnp.float32))
            outer[t, quad * 2 * KP : (quad + 1) * 2 * KP, :] = jnp.concatenate(
                halves, axis=0
            ).astype(jnp.bfloat16)
        return carry

    lax.fori_loop(0, trip, contract_a, 0)

    spot = lax.broadcasted_iota(jnp.int32, (sent, sent), 0)
    order = lane_iota((sent, sent)) == spot % n * slots + spot // n
    places[...] = jnp.dot(
        order.astype(jnp.bfloat16), hot_send, preferred_element_type=jnp.float32
    ).astype(jnp.bfloat16)

    at = freq_at - low
    scale = math.sqrt(math.log2(math.e)) / smear_width
    part_freq = pltpu.roll(part_tiles(low // LANES), LANES - at, 1)
    near_freq = pltpu.roll(near_tiles(low // LANES), LANES - at, 1)
    part_freq = jnp.where(lane_iota(part_freq.shape) < nb, part_freq, 1.0)
    part_scaled, part_log = part_freq * scale, -jnp.log2(part_freq)
    first_half = lane_iota((8, LANES)) < IM
    for t in range(trip):
        for pair in range(nb // 2):
            at_row = (t * (nb // 2) + pair) * 8
            for into, of in ((second, part_scaled), (third, part_log)):
                even = jnp.broadcast_to(of[t : t + 1, 2 * pair : 2 * pair + 1], (8, LANES))
                odd = jnp.broadcast_to(
                    of[t : t + 1, 2 * pair + 1 : 2 * pair + 2], (8, LANES)
                )
                into[at_row : at_row + 8, :] = jnp.where(first_half, even, odd)
    near_col = jnp.transpose(
        jnp.concatenate([near_freq, jnp.ones((LANES - trip, LANES), jnp.float32)], axis=0)
    )[0:KP]

    recv[me] = send_ref[me]

    all_moved(recv, send_sem)
    all_moved(recv, recv_sem)

    for t in range(trip):
        where = slot_s[t]
        pair = recv[where // slots].astype(jnp.float32)
        row = pair[0:1]
        for s in range(1, slots):
            row = jnp.where(where % slots == s, pair[s : s + 1], row)
        far_rows[t : t + 1, :] = row

    far_tiles = tiles_of(far_rows)
    spread_rows(far_tiles, nb, far_mat, IM, True)
    far_freq = pltpu.roll(far_tiles(low // LANES), LANES - at, 1)
    lanes = lane_iota(far_freq.shape)
    far_freq = jnp.where(lanes < IM, far_freq, pltpu.roll(far_freq, IM, 1))
    used = (lanes % IM) < nb
    far_freq = jnp.where(used, far_freq, 1.0)
    used_cell = (lax.broadcasted_iota(jnp.int32, (KP, LANES), 0) < nb) & (
        lane_iota((KP, LANES)) % IM < nb
    )
    live = live_s[0]

    for t in range(trip):
        ef_re = far_mat[pl.ds(t, KP, stride=trip), :].astype(jnp.bfloat16)
        ef_im = far_mat[pl.ds(KP * trip + t, KP, stride=trip), :].astype(jnp.bfloat16)
        zero = jnp.zeros((IM, LANES), jnp.bfloat16)
        cols = []
        for ef in (ef_re, ef_im):
            ef = jnp.concatenate([ef, zero[0 : IM - KP]], axis=0)
            cols.append(jnp.concatenate([ef, zero], axis=1))
            cols.append(jnp.concatenate([zero, ef], axis=1))
        ef = jnp.concatenate(cols, axis=0)
        w1 = jnp.broadcast_to(near_col[:, t : t + 1], (KP, LANES))
        w3 = jnp.broadcast_to(far_freq[t : t + 1, :], (KP, LANES))
        base = (w1 - w3) * scale
        total = jnp.zeros((KP, LANES), jnp.float32)
        v = lax.dot_general(
            outer[t], ef, (((1,), (1,)), ((), ())), preferred_element_type=jnp.float32
        )
        for pair in range(nb // 2):
            at_row = (t * (nb // 2) + pair) * 8
            w2 = jnp.concatenate([second[at_row : at_row + 8, :]] * (KP // 8), axis=0)
            log = jnp.concatenate([third[at_row : at_row + 8, :]] * (KP // 8), axis=0)
            re = v[pair * KP : (pair + 1) * KP, 0:LANES]
            im = v[pair * KP : (pair + 1) * KP, LANES : 2 * LANES]
            x = base + w2
            total = total + (re * re + im * im) * jnp.exp2(log - x * x)
        keep = used_cell & (t < live)
        total = jnp.where(keep, total / (w1 * w3 * nb), 0.0)
        near_sum = jnp.sum(total, axis=1, keepdims=True)
        near_acc[t] = jnp.broadcast_to(near_sum, (KP, LANES))
        far_sum = jnp.sum(total, axis=0, keepdims=True)
        far_sum = far_sum + pltpu.roll(far_sum, IM, 1)
        far_acc[t : t + 1, :] = jnp.where(lane_iota(far_sum.shape) < nb, far_sum, 0.0)

    spots = lax.broadcasted_iota(jnp.int32, (n, LANES), 0)
    back = jnp.zeros((n, LANES), jnp.float32)
    for t in range(trip):
        where = slot_s[t]
        row = far_acc[t : t + 1, :]
        for s in range(1, slots):
            row = jnp.where(where % slots == s, pltpu.roll(row, s * LANES // slots, 1), row)
        back = back + jnp.where(spots == where // slots, row, 0.0)
    by_slot[...] = back.reshape(n, 1, LANES)
    returned[me] = by_slot[me]

    def begin_back(i, carry):
        give_back(i).start()
        return carry

    lax.fori_loop(0, n - 1, begin_back, 0)

    columns = lane_iota((1, owned))
    rates = jnp.zeros((KP, owned), jnp.float32)
    for t in range(trip):
        spread = jnp.concatenate([near_acc[t]] * (owned // LANES), axis=1)
        rates = rates + jnp.where(columns == local_ref[0:1, t : t + 1], spread, 0.0)

    all_moved(returned, back_send)
    all_moved(returned, back_recv)

    filled = returned[...].reshape(n, LANES)
    filled = jnp.concatenate(
        [filled] + [pltpu.roll(filled, LANES - s * LANES // slots, 1) for s in range(1, slots)],
        axis=0,
    )
    filled = jnp.transpose(filled)[0:KP]
    parts = []
    for _ in range(3):
        part = filled.astype(jnp.bfloat16)
        parts.append(part)
        filled = filled - part.astype(jnp.float32)
    placed = jnp.dot(
        jnp.concatenate(parts, axis=0), places[...], preferred_element_type=jnp.float32
    )
    for i in range(3):
        rates = rates + placed[i * KP : (i + 1) * KP]
    out_ref[...] = rates[0:nb]


def on_device(n, eigvec, omega, phi, send_rows, local_q, partner_q, slot_ref, tri_count):
    owned = eigvec.shape[0]
    nb = omega.shape[1]
    trip = local_q.shape[0]
    slots = send_rows.shape[1] // n
    width = -(-(eigvec.shape[1] + nb) // LANES) * LANES
    vmem = pl.BlockSpec(memory_space=pltpu.VMEM)
    hbm = pl.BlockSpec(memory_space=pl.ANY)
    smem = pl.BlockSpec(memory_space=pltpu.SMEM)
    f32 = jnp.float32
    return pl.pallas_call(
        functools.partial(rate_kernel, n, nb, slots),
        out_shape=jax.ShapeDtypeStruct((nb, owned), f32),
        in_specs=[hbm, vmem, hbm] + [vmem] * 3 + [smem] * 2,
        out_specs=vmem,
        scratch_shapes=[
            pltpu.VMEM((eigvec.shape[1], owned), jnp.bfloat16),
            pltpu.VMEM(phi.shape, jnp.bfloat16),
            pltpu.VMEM((n, slots, width), jnp.bfloat16),
            pltpu.VMEM((trip, width), f32),
            pltpu.VMEM((trip, width), f32),
            pltpu.VMEM((n * slots, owned), jnp.bfloat16),
            pltpu.VMEM((n, slots, width), jnp.bfloat16),
            pltpu.VMEM((2 * KP * trip, LANES), f32),
            pltpu.VMEM((KP * trip, LANES), f32),
            pltpu.VMEM((2 * KP * trip, LANES), f32),
            pltpu.VMEM((trip, width), f32),
            pltpu.VMEM((2 * KP * (nb * trip + 8), LANES), f32),
            pltpu.VMEM((trip, nb // 2 * KP, 2 * LANES), jnp.bfloat16),
            pltpu.VMEM((trip * nb // 2 * 8, LANES), f32),
            pltpu.VMEM((trip * nb // 2 * 8, LANES), f32),
            pltpu.VMEM((trip, KP, LANES), f32),
            pltpu.VMEM((trip, LANES), f32),
            pltpu.VMEM((n, 1, LANES), f32),
            pltpu.VMEM((n, 1, LANES), f32),
            pltpu.SemaphoreType.DMA((1,)),
            pltpu.SemaphoreType.DMA((1,)),
            pltpu.SemaphoreType.DMA((1,)),
            pltpu.SemaphoreType.DMA((1,)),
            pltpu.SemaphoreType.DMA((2,)),
        ],
        compiler_params=pltpu.CompilerParams(
            collective_id=0, has_side_effects=True, vmem_limit_bytes=60 * 1024 * 1024
        ),
    )(
        eigvec.T,
        omega.T,
        phi,
        send_rows,
        local_q.reshape(1, trip),
        partner_q.reshape(1, trip),
        slot_ref,
        tri_count,
    )


def solution(mesh):
    in_specs = (
        P(("groups", "pb"), None),
        P(("groups", "pb"), None),
        P(),
        P(("groups", "pb"), None),
        P(("groups", "pb")),
        P(("groups", "pb")),
        P(("groups", "pb")),
        P(("groups", "pb")),
    )
    out_specs = P(None, ("groups", "pb"))
    return jax.shard_map(
        functools.partial(on_device, mesh.shape["pb"]),
        mesh=mesh,
        in_specs=in_specs,
        out_specs=out_specs,
        check_vma=False,
    )
```

```python
import functools
import math

import jax
import jax.numpy as jnp
from jax import lax
from jax.experimental import pallas as pl
from jax.experimental.pallas import tpu as pltpu
from jax.sharding import PartitionSpec as P

LANES = 128
IM = 64
AHEAD = 2
KP = 40
smear_width = 0.5
MESH = pl.DeviceIdType.MESH


def lane_iota(shape):
    return lax.broadcasted_iota(jnp.int32, shape, len(shape) - 1)


def shifted_window(tiles, start, width, to):
    first, at = divmod(start, LANES)
    moved = pltpu.roll(tiles(first), (to - at) % LANES, 1) if to != at else tiles(first)
    if at + width > LANES:
        after = pltpu.roll(tiles(first + 1), (to - at) % LANES, 1)
        moved = jnp.where(lane_iota(moved.shape) < to + LANES - at, moved, after)
    return moved


def spread_rows(tiles, nb, out_ref, im_at, both):
    half = nb * nb

    def put(k, value):
        count = value.shape[0]
        out_ref[k * count : (k + 1) * count, :] = value

    for k in range(nb):
        re = shifted_window(tiles, k * nb, nb, 0)
        im = shifted_window(tiles, half + k * nb, nb, im_at)
        lanes = lane_iota(re.shape)
        in_re = lanes < nb
        in_im = (lanes >= im_at) & (lanes < im_at + nb)
        put(k, jnp.where(in_re, re, jnp.where(in_im, im, 0.0)))
        if both:
            im0 = shifted_window(tiles, half + k * nb, nb, 0)
            re1 = shifted_window(tiles, k * nb, nb, im_at)
            put(KP + k, jnp.where(in_re, -im0, jnp.where(in_im, re1, 0.0)))
    zero = jnp.zeros(re.shape, jnp.float32)
    for k in range(nb, KP):
        put(k, zero)
        if both:
            put(KP + k, zero)


def picked(index_row, count):
    width = index_row.shape[1]
    hot = lax.broadcasted_iota(jnp.int32, (count, width), 0) == index_row
    return hot.astype(jnp.float32)


def waves_of(n):
    half = n // 4
    far, mid = half // 2 + 1, max(1, half // 4)
    return [w for w in ((far, half), (mid, far - 1), (0, mid - 1)) if w[0] <= w[1]]


def wave_rows(n, wave):
    near, far = wave
    chips = 2 * (far - near + 1) - (near == 0) - (far == n // 4)
    return 2 * chips


def rate_kernel(
    n,
    nb,
    slots,
    eig_hbm,
    omega_hbm,
    phi_hbm,
    rows_hbm,
    local_hbm,
    partner_hbm,
    slot_hbm,
    live_hbm,
    out_ref,
    eig_ref,
    omega_ref,
    phi_ref,
    rows_ref,
    local_ref,
    partner_ref,
    slot_s,
    live_s,
    send_ref,
    near_ref,
    part_ref,
    places,
    recvs,
    mat,
    near_mat,
    far_mat,
    far_rows,
    inner,
    outer,
    second,
    third,
    near_acc,
    far_acc,
    by_slots,
    returned,
    send_sem,
    recv_sem,
    back_send,
    back_recv,
    load_sem,
):
    me = lax.axis_index("pb")
    trip = near_ref.shape[0]
    owned = out_ref.shape[1]
    freq_at = 2 * nb * nb
    quads = nb // 4

    chips = n // 2
    half = chips // 2
    chip, core = me // 2, lax.rem(me, 2)
    waves = waves_of(n)

    def each(far, near, act):
        if far == half:
            act(half, 0)
            act(half, 1)
            far -= 1
        last = max(near, 1)
        if far >= last:

            def step(i, carry):
                d = far - i // 4
                act(jnp.where(i % 4 < 2, d, chips - d), i % 2)
                return carry

            lax.fori_loop(0, 4 * (far - last + 1), step, 0)
        if near == 0:
            act(0, 1)

    def device(r, c):
        return lax.rem(chip + r, chips) * 2 + lax.rem(core + c, 2)

    def seat(wave, r, c):
        near, far = waves[wave]
        first = far - near + 1
        back = chips - min(far, half - 1)
        second = chips - max(near, 1)
        low_side = (r >= near) & (r <= far)
        high_side = (r >= back) & (r <= second)
        row = jnp.where(low_side, r - near, jnp.where(high_side, first + r - back, 0))
        return row * 2 + c, low_side | high_side

    def moved(ref, count, sem):
        every = ref.at[pl.ds(0, count)]
        pltpu.make_async_copy(every, every, sem).wait()

    def exchange(wave):
        def act(r, c):
            to = device(r, c)
            row, _ = seat(wave, lax.rem(chips - r, chips), c)
            pltpu.make_async_remote_copy(
                src_ref=send_ref.at[to],
                dst_ref=recvs[wave].at[row],
                send_sem=send_sem.at[0],
                recv_sem=recv_sem.at[wave],
                device_id={"pb": to},
                device_id_type=MESH,
            ).start()

        return act

    def give_back(wave):
        def act(r, c):
            to = device(r, c)
            pltpu.make_async_remote_copy(
                src_ref=by_slots[wave].at[to],
                dst_ref=returned.at[me],
                send_sem=back_send.at[0],
                recv_sem=back_recv.at[0],
                device_id={"pb": to},
                device_id_type=MESH,
            ).start()

        return act

    load_eig = pltpu.make_async_copy(eig_hbm, eig_ref, load_sem.at[0])
    load_phi = pltpu.make_async_copy(phi_hbm, phi_ref, load_sem.at[1])
    small = (
        (rows_hbm, rows_ref),
        (local_hbm, local_ref),
        (partner_hbm, partner_ref),
        (omega_hbm, omega_ref),
        (slot_hbm, slot_s),
        (live_hbm, live_s),
    )
    loads = [
        pltpu.make_async_copy(source, into, load_sem.at[2 + i])
        for i, (source, into) in enumerate(small)
    ]
    for load in loads + [load_eig, load_phi]:
        load.start()
    barrier = pltpu.get_barrier_semaphore()

    def greet(r, c):
        pl.semaphore_signal(
            barrier, inc=1, device_id={"pb": device(r, c)}, device_id_type=MESH
        )

    each(half, 0, greet)
    for load in loads:
        load.wait()

    rest = jnp.full((1, LANES - 2 * trip), -1, jnp.int32)
    own_row = jnp.concatenate([local_ref[...], partner_ref[...], rest], axis=1)
    hot_send = jnp.transpose(picked(rows_ref[...], owned)).astype(jnp.bfloat16)
    hot_own = jnp.transpose(picked(own_row, owned))[0 : 2 * trip].astype(jnp.bfloat16)
    hot = jnp.concatenate([hot_send, hot_own], axis=0)
    sent = n * slots
    load_eig.wait()
    low = freq_at // LANES * LANES
    tail = jnp.concatenate(
        [
            eig_ref[low:freq_at, :].astype(jnp.float32),
            omega_ref[...].astype(jnp.float32),
            jnp.zeros((low + LANES - freq_at - nb, owned), jnp.float32),
        ],
        axis=0,
    ).astype(jnp.bfloat16)
    piece = 2 * LANES
    for start in range(0, low + LANES, piece):
        end = min(start + piece, low + LANES)
        table = tail if start == low else eig_ref[start:end, :]
        rows = lax.dot_general(
            hot, table, (((1,), (1,)), ((), ())), preferred_element_type=jnp.float32
        )
        send_ref[:, :, start:end] = (
            rows[0:sent].astype(jnp.bfloat16).reshape(n, slots, end - start)
        )
        near_ref[:, start:end] = rows[sent : sent + trip]
        part_ref[:, start:end] = rows[sent + trip : sent + 2 * trip]

    pl.semaphore_wait(barrier, n - 1)

    for wave, (near, far) in enumerate(waves[:2]):
        each(far, near if wave == 0 else max(near, far - AHEAD + 1), exchange(wave))

    def tiles_of(ref):
        return lambda k: ref[:, k * LANES : (k + 1) * LANES]

    near_tiles, part_tiles = tiles_of(near_ref), tiles_of(part_ref)
    spread_rows(part_tiles, nb, mat, IM, True)
    spread_rows(near_tiles, nb, near_mat, KP, False)

    rows = nb * trip
    pitch = inner.shape[0] // (2 * KP)
    zero_rows = jnp.zeros(((KP - nb) * pitch, LANES), jnp.float32)
    inner[nb * pitch : KP * pitch, :] = zero_rows
    inner[(KP + nb) * pitch : 2 * KP * pitch, :] = zero_rows
    part_re = mat[0:rows, :].astype(jnp.bfloat16)
    part_im = mat[KP * trip : KP * trip + rows, :].astype(jnp.bfloat16)

    def contract_b(a, carry):
        block = phi_ref[a].astype(jnp.float32)
        block = jnp.concatenate([block, jnp.zeros((nb, LANES - nb), jnp.float32)], axis=1)
        block = jnp.concatenate([block, jnp.zeros((KP - nb, LANES), jnp.float32)], axis=0)
        gap = jnp.zeros((IM - KP, LANES), jnp.float32)
        block = jnp.concatenate([block, gap, pltpu.roll(block, IM, 1), gap], axis=0)
        block = block.astype(jnp.bfloat16)
        for part, first in ((part_re, 0), (part_im, KP)):
            at = pl.multiple_of((first + a) * pitch, 8)
            inner[pl.ds(at, rows), :] = jnp.dot(
                part, block, preferred_element_type=jnp.float32
            )
        return carry

    load_phi.wait()
    lax.fori_loop(0, nb, contract_b, 0)

    def contract_a(t, carry):
        left = near_mat[pl.ds(t, KP, stride=trip), :]
        left = left[:, 0 : 2 * KP].astype(jnp.bfloat16)
        for quad in range(quads):
            halves = []
            for pair in range(2):
                sides = []
                for one in range(2):
                    m = quad * 4 + pair * 2 + one
                    sides.append(
                        inner[pl.ds(m * trip + t, 2 * KP, stride=pitch), :].astype(
                            jnp.bfloat16
                        )
                    )
                right = jnp.concatenate(sides, axis=1)
                halves.append(jnp.dot(left, right, preferred_element_type=jnp.float32))
            outer[t, quad * 2 * KP : (quad + 1) * 2 * KP, :] = jnp.concatenate(
                halves, axis=0
            ).astype(jnp.bfloat16)
        return carry

    lax.fori_loop(0, trip, contract_a, 0)

    spot = lax.broadcasted_iota(jnp.int32, (sent, sent), 0)
    order = lane_iota((sent, sent)) == spot % n * slots + spot // n
    places[...] = jnp.dot(
        order.astype(jnp.bfloat16), hot_send, preferred_element_type=jnp.float32
    ).astype(jnp.bfloat16)

    at = freq_at - low
    scale = math.sqrt(math.log2(math.e)) / smear_width
    part_freq = pltpu.roll(part_tiles(low // LANES), LANES - at, 1)
    near_freq = pltpu.roll(near_tiles(low // LANES), LANES - at, 1)
    part_freq = jnp.where(lane_iota(part_freq.shape) < nb, part_freq, 1.0)
    part_scaled, part_log = part_freq * scale, -jnp.log2(part_freq)
    first_half = lane_iota((8, LANES)) < IM
    for t in range(trip):
        for pair in range(nb // 2):
            at_row = (t * (nb // 2) + pair) * 8
            for into, of in ((second, part_scaled), (third, part_log)):
                even = jnp.broadcast_to(of[t : t + 1, 2 * pair : 2 * pair + 1], (8, LANES))
                odd = jnp.broadcast_to(
                    of[t : t + 1, 2 * pair + 1 : 2 * pair + 2], (8, LANES)
                )
                into[at_row : at_row + 8, :] = jnp.where(first_half, even, odd)
    near_col = jnp.transpose(
        jnp.concatenate([near_freq, jnp.ones((LANES - trip, LANES), jnp.float32)], axis=0)
    )[0:KP]

    for wave, (near, far) in enumerate(waves):
        count = recvs[wave].shape[0]
        if near == 0:
            recvs[wave][0] = send_ref[me]
            count -= 1
        moved(recvs[wave] if near else send_ref, count, recv_sem.at[wave])
        in_wave = []
        for t in range(trip):
            where = slot_s[t]
            owner = where // slots
            seat_of, here = seat(
                wave,
                lax.rem(owner // 2 - chip + chips, chips),
                lax.rem(owner + core, 2),
            )
            in_wave.append(here)
            pair = recvs[wave][seat_of].astype(jnp.float32)
            row = pair[0:1]
            for s in range(1, slots):
                row = jnp.where(where % slots == s, pair[s : s + 1], row)
            far_rows[t : t + 1, :] = row

        far_tiles = tiles_of(far_rows)
        spread_rows(far_tiles, nb, far_mat, IM, True)
        far_freq = pltpu.roll(far_tiles(low // LANES), LANES - at, 1)
        lanes = lane_iota(far_freq.shape)
        far_freq = jnp.where(lanes < IM, far_freq, pltpu.roll(far_freq, IM, 1))
        used = (lanes % IM) < nb
        far_freq = jnp.where(used, far_freq, 1.0)
        used_cell = (lax.broadcasted_iota(jnp.int32, (KP, LANES), 0) < nb) & (
            lane_iota((KP, LANES)) % IM < nb
        )
        live = live_s[0]

        for t in range(trip):
            ef_re = far_mat[pl.ds(t, KP, stride=trip), :].astype(jnp.bfloat16)
            ef_im = far_mat[pl.ds(KP * trip + t, KP, stride=trip), :].astype(jnp.bfloat16)
            zero = jnp.zeros((IM, LANES), jnp.bfloat16)
            cols = []
            for ef in (ef_re, ef_im):
                ef = jnp.concatenate([ef, zero[0 : IM - KP]], axis=0)
                cols.append(jnp.concatenate([ef, zero], axis=1))
                cols.append(jnp.concatenate([zero, ef], axis=1))
            ef = jnp.concatenate(cols, axis=0)
            w1 = jnp.broadcast_to(near_col[:, t : t + 1], (KP, LANES))
            w3 = jnp.broadcast_to(far_freq[t : t + 1, :], (KP, LANES))
            base = (w1 - w3) * scale
            total = jnp.zeros((KP, LANES), jnp.float32)
            v = lax.dot_general(
                outer[t], ef, (((1,), (1,)), ((), ())), preferred_element_type=jnp.float32
            )
            for pair in range(nb // 2):
                at_row = (t * (nb // 2) + pair) * 8
                w2 = jnp.concatenate([second[at_row : at_row + 8, :]] * (KP // 8), axis=0)
                log = jnp.concatenate([third[at_row : at_row + 8, :]] * (KP // 8), axis=0)
                re = v[pair * KP : (pair + 1) * KP, 0:LANES]
                im = v[pair * KP : (pair + 1) * KP, LANES : 2 * LANES]
                x = base + w2
                total = total + (re * re + im * im) * jnp.exp2(log - x * x)
            keep = used_cell & (in_wave[t] & (t < live))
            total = jnp.where(keep, total / (w1 * w3 * nb), 0.0)
            near_sum = jnp.sum(total, axis=1, keepdims=True)
            near_sum = jnp.broadcast_to(near_sum, (KP, LANES))
            near_acc[t] = near_sum if wave == 0 else near_acc[t] + near_sum
            far_sum = jnp.sum(total, axis=0, keepdims=True)
            far_sum = far_sum + pltpu.roll(far_sum, IM, 1)
            far_acc[t : t + 1, :] = jnp.where(lane_iota(far_sum.shape) < nb, far_sum, 0.0)

        spots = lax.broadcasted_iota(jnp.int32, (n, LANES), 0)
        back = jnp.zeros((n, LANES), jnp.float32)
        for t in range(trip):
            where = slot_s[t]
            row = far_acc[t : t + 1, :]
            for s in range(1, slots):
                row = jnp.where(where % slots == s, pltpu.roll(row, s * LANES // slots, 1), row)
            back = back + jnp.where(spots == where // slots, row, 0.0)
        by_slots[wave][...] = back.reshape(n, 1, LANES)
        if near == 0:
            returned[me] = by_slots[wave][me]
        each(far, near, give_back(wave))
        if wave == 0:
            for later, (start, stop) in enumerate(waves):
                if later == 1 and stop - AHEAD >= start:
                    each(stop - AHEAD, start, exchange(later))
                elif later > 1:
                    each(stop, start, exchange(later))
    moved(send_ref, n - 1, send_sem.at[0])

    columns = lane_iota((1, owned))
    rates = jnp.zeros((KP, owned), jnp.float32)
    for t in range(trip):
        spread = jnp.concatenate([near_acc[t]] * (owned // LANES), axis=1)
        rates = rates + jnp.where(columns == local_ref[0:1, t : t + 1], spread, 0.0)

    moved(returned, n - 1, back_send.at[0])
    moved(returned, n - 1, back_recv.at[0])

    filled = returned[...].reshape(n, LANES)
    filled = jnp.concatenate(
        [filled] + [pltpu.roll(filled, LANES - s * LANES // slots, 1) for s in range(1, slots)],
        axis=0,
    )
    filled = jnp.transpose(filled)[0:KP]
    parts = []
    for _ in range(3):
        part = filled.astype(jnp.bfloat16)
        parts.append(part)
        filled = filled - part.astype(jnp.float32)
    placed = jnp.dot(
        jnp.concatenate(parts, axis=0), places[...], preferred_element_type=jnp.float32
    )
    for i in range(3):
        rates = rates + placed[i * KP : (i + 1) * KP]
    out_ref[...] = rates[0:nb]


def on_device(n, eigvec, omega, phi, send_rows, local_q, partner_q, slot_ref, tri_count):
    owned = eigvec.shape[0]
    nb = omega.shape[1]
    trip = local_q.shape[0]
    slots = send_rows.shape[1] // n
    width = -(-(eigvec.shape[1] + nb) // LANES) * LANES
    vmem = pl.BlockSpec(memory_space=pltpu.VMEM)
    hbm = pl.BlockSpec(memory_space=pl.ANY)
    f32 = jnp.float32
    waves = waves_of(n)
    return pl.pallas_call(
        functools.partial(rate_kernel, n, nb, slots),
        out_shape=jax.ShapeDtypeStruct((nb, owned), f32),
        in_specs=[hbm] * 8,
        out_specs=vmem,
        scratch_shapes=[
            pltpu.VMEM((eigvec.shape[1], owned), jnp.bfloat16),
            pltpu.VMEM((nb, owned), jnp.bfloat16),
            pltpu.VMEM(phi.shape, jnp.bfloat16),
            pltpu.VMEM(send_rows.shape, jnp.int32),
            pltpu.VMEM((1, trip), jnp.int32),
            pltpu.VMEM((1, trip), jnp.int32),
            pltpu.SMEM((trip,), jnp.int32),
            pltpu.SMEM((1,), jnp.int32),
            pltpu.VMEM((n, slots, width), jnp.bfloat16),
            pltpu.VMEM((trip, width), f32),
            pltpu.VMEM((trip, width), f32),
            pltpu.VMEM((n * slots, owned), jnp.bfloat16),
            [pltpu.VMEM((wave_rows(n, w), slots, width), jnp.bfloat16) for w in waves],
            pltpu.VMEM((2 * KP * trip, LANES), f32),
            pltpu.VMEM((KP * trip, LANES), f32),
            pltpu.VMEM((2 * KP * trip, LANES), f32),
            pltpu.VMEM((trip, width), f32),
            pltpu.VMEM((2 * KP * (nb * trip + 8), LANES), f32),
            pltpu.VMEM((trip, nb // 2 * KP, 2 * LANES), jnp.bfloat16),
            pltpu.VMEM((trip * nb // 2 * 8, LANES), f32),
            pltpu.VMEM((trip * nb // 2 * 8, LANES), f32),
            pltpu.VMEM((trip, KP, LANES), f32),
            pltpu.VMEM((trip, LANES), f32),
            [pltpu.VMEM((n, 1, LANES), f32) for _ in waves],
            pltpu.VMEM((n, 1, LANES), f32),
            pltpu.SemaphoreType.DMA((1,)),
            pltpu.SemaphoreType.DMA((len(waves),)),
            pltpu.SemaphoreType.DMA((1,)),
            pltpu.SemaphoreType.DMA((1,)),
            pltpu.SemaphoreType.DMA((8,)),
        ],
        compiler_params=pltpu.CompilerParams(
            collective_id=0, has_side_effects=True, vmem_limit_bytes=60 * 1024 * 1024
        ),
    )(
        eigvec.T,
        omega.T,
        phi,
        send_rows,
        local_q.reshape(1, trip),
        partner_q.reshape(1, trip),
        slot_ref,
        tri_count,
    )


def solution(mesh):
    in_specs = (
        P(("groups", "pb"), None),
        P(("groups", "pb"), None),
        P(),
        P(("groups", "pb"), None),
        P(("groups", "pb")),
        P(("groups", "pb")),
        P(("groups", "pb")),
        P(("groups", "pb")),
    )
    out_specs = P(None, ("groups", "pb"))
    return jax.shard_map(
        functools.partial(on_device, mesh.shape["pb"]),
        mesh=mesh,
        in_specs=in_specs,
        out_specs=out_specs,
        check_vma=False,
    )
```

```python
import functools
import math

import jax
import jax.numpy as jnp
from jax import lax
from jax.experimental import pallas as pl
from jax.experimental.pallas import tpu as pltpu
from jax.sharding import PartitionSpec as P

LANES = 128
IM = 64
KP = 40
smear_width = 0.5
MESH = pl.DeviceIdType.MESH


def lane_iota(shape):
    return lax.broadcasted_iota(jnp.int32, shape, len(shape) - 1)


def shifted_window(tiles, start, width, to):
    first, at = divmod(start, LANES)
    moved = pltpu.roll(tiles(first), (to - at) % LANES, 1) if to != at else tiles(first)
    if at + width > LANES:
        after = pltpu.roll(tiles(first + 1), (to - at) % LANES, 1)
        moved = jnp.where(lane_iota(moved.shape) < to + LANES - at, moved, after)
    return moved


def spread_rows(tiles, nb, out_ref, im_at, both):
    half = nb * nb

    def put(k, value):
        count = value.shape[0]
        out_ref[k * count : (k + 1) * count, :] = value

    for k in range(nb):
        re = shifted_window(tiles, k * nb, nb, 0)
        im = shifted_window(tiles, half + k * nb, nb, im_at)
        lanes = lane_iota(re.shape)
        in_re = lanes < nb
        in_im = (lanes >= im_at) & (lanes < im_at + nb)
        put(k, jnp.where(in_re, re, jnp.where(in_im, im, 0.0)))
        if both:
            im0 = shifted_window(tiles, half + k * nb, nb, 0)
            re1 = shifted_window(tiles, k * nb, nb, im_at)
            put(KP + k, jnp.where(in_re, -im0, jnp.where(in_im, re1, 0.0)))
    zero = jnp.zeros(re.shape, jnp.float32)
    for k in range(nb, KP):
        put(k, zero)
        if both:
            put(KP + k, zero)


def picked(index_row, count):
    width = index_row.shape[1]
    hot = lax.broadcasted_iota(jnp.int32, (count, width), 0) == index_row
    return hot.astype(jnp.float32)


def waves_of(n):
    half = n // 4
    far, mid = half // 2 + 1, max(1, half // 4)
    return [w for w in ((far, half), (mid, far - 1), (0, mid - 1)) if w[0] <= w[1]]


def wave_rows(n, wave):
    near, far = wave
    chips = 2 * (far - near + 1) - (near == 0) - (far == n // 4)
    return 2 * chips


def rate_kernel(
    n,
    nb,
    slots,
    eig_hbm,
    omega_hbm,
    phi_hbm,
    rows_hbm,
    local_hbm,
    partner_hbm,
    slot_hbm,
    live_hbm,
    out_ref,
    eig_ref,
    omega_ref,
    phi_ref,
    rows_ref,
    local_ref,
    partner_ref,
    slot_s,
    live_s,
    send_ref,
    near_ref,
    part_ref,
    places,
    recvs,
    mat,
    near_mat,
    far_mat,
    far_rows,
    inner,
    outer,
    second,
    third,
    near_acc,
    far_acc,
    by_slots,
    returned,
    send_sem,
    recv_sem,
    back_send,
    back_recv,
    load_sem,
):
    me = lax.axis_index("pb")
    trip = near_ref.shape[0]
    owned = out_ref.shape[1]
    freq_at = 2 * nb * nb
    quads = nb // 4

    chips = n // 2
    half = chips // 2
    chip, core = me // 2, lax.rem(me, 2)
    waves = waves_of(n)

    def each(far, near, act):
        if far == half:
            act(half, 0)
            act(half, 1)
            far -= 1
        last = max(near, 1)
        if far >= last:

            def step(i, carry):
                d = far - i // 4
                act(jnp.where(i % 4 < 2, d, chips - d), i % 2)
                return carry

            lax.fori_loop(0, 4 * (far - last + 1), step, 0)
        if near == 0:
            act(0, 1)

    def device(r, c):
        return lax.rem(chip + r, chips) * 2 + lax.rem(core + c, 2)

    def seat(wave, r, c):
        near, far = waves[wave]
        first = far - near + 1
        back = chips - min(far, half - 1)
        second = chips - max(near, 1)
        low_side = (r >= near) & (r <= far)
        high_side = (r >= back) & (r <= second)
        row = jnp.where(low_side, r - near, jnp.where(high_side, first + r - back, 0))
        return row * 2 + c, low_side | high_side

    def moved(ref, count, sem):
        every = ref.at[pl.ds(0, count)]
        pltpu.make_async_copy(every, every, sem).wait()

    def exchange(wave):
        def act(r, c):
            to = device(r, c)
            row, _ = seat(wave, lax.rem(chips - r, chips), c)
            pltpu.make_async_remote_copy(
                src_ref=send_ref.at[to],
                dst_ref=recvs[wave].at[row],
                send_sem=send_sem.at[0],
                recv_sem=recv_sem.at[wave],
                device_id={"pb": to},
                device_id_type=MESH,
            ).start()

        return act

    def give_back(wave):
        def act(r, c):
            to = device(r, c)
            pltpu.make_async_remote_copy(
                src_ref=by_slots[wave].at[to],
                dst_ref=returned.at[me],
                send_sem=back_send.at[0],
                recv_sem=back_recv.at[0],
                device_id={"pb": to},
                device_id_type=MESH,
            ).start()

        return act

    load_eig = pltpu.make_async_copy(eig_hbm, eig_ref, load_sem.at[0])
    load_phi = pltpu.make_async_copy(phi_hbm, phi_ref, load_sem.at[1])
    small = (
        (rows_hbm, rows_ref),
        (local_hbm, local_ref),
        (partner_hbm, partner_ref),
        (omega_hbm, omega_ref),
        (slot_hbm, slot_s),
        (live_hbm, live_s),
    )
    loads = [
        pltpu.make_async_copy(source, into, load_sem.at[2 + i])
        for i, (source, into) in enumerate(small)
    ]
    for load in loads + [load_eig, load_phi]:
        load.start()
    barrier = pltpu.get_barrier_semaphore()

    def greet(r, c):
        pl.semaphore_signal(
            barrier, inc=1, device_id={"pb": device(r, c)}, device_id_type=MESH
        )

    each(half, 0, greet)
    for load in loads:
        load.wait()

    rest = jnp.full((1, LANES - 2 * trip), -1, jnp.int32)
    own_row = jnp.concatenate([local_ref[...], partner_ref[...], rest], axis=1)
    hot_send = jnp.transpose(picked(rows_ref[...], owned)).astype(jnp.bfloat16)
    hot_own = jnp.transpose(picked(own_row, owned))[0 : 2 * trip].astype(jnp.bfloat16)
    hot = jnp.concatenate([hot_send, hot_own], axis=0)
    sent = n * slots
    load_eig.wait()
    low = freq_at // LANES * LANES
    tail = jnp.concatenate(
        [
            eig_ref[low:freq_at, :].astype(jnp.float32),
            omega_ref[...].astype(jnp.float32),
            jnp.zeros((low + LANES - freq_at - nb, owned), jnp.float32),
        ],
        axis=0,
    ).astype(jnp.bfloat16)
    piece = 2 * LANES
    for start in range(0, low + LANES, piece):
        end = min(start + piece, low + LANES)
        table = tail if start == low else eig_ref[start:end, :]
        rows = lax.dot_general(
            hot, table, (((1,), (1,)), ((), ())), preferred_element_type=jnp.float32
        )
        send_ref[:, :, start:end] = (
            rows[0:sent].astype(jnp.bfloat16).reshape(n, slots, end - start)
        )
        near_ref[:, start:end] = rows[sent : sent + trip]
        part_ref[:, start:end] = rows[sent + trip : sent + 2 * trip]

    pl.semaphore_wait(barrier, n - 1)

    for wave, (near, far) in enumerate(waves):
        each(far, near, exchange(wave))

    def tiles_of(ref):
        return lambda k: ref[:, k * LANES : (k + 1) * LANES]

    near_tiles, part_tiles = tiles_of(near_ref), tiles_of(part_ref)
    spread_rows(part_tiles, nb, mat, IM, True)
    spread_rows(near_tiles, nb, near_mat, KP, False)

    rows = nb * trip
    pitch = inner.shape[0] // (2 * KP)
    zero_rows = jnp.zeros(((KP - nb) * pitch, LANES), jnp.float32)
    inner[nb * pitch : KP * pitch, :] = zero_rows
    inner[(KP + nb) * pitch : 2 * KP * pitch, :] = zero_rows
    part_re = mat[0:rows, :].astype(jnp.bfloat16)
    part_im = mat[KP * trip : KP * trip + rows, :].astype(jnp.bfloat16)

    def contract_b(a, carry):
        block = phi_ref[a].astype(jnp.float32)
        block = jnp.concatenate([block, jnp.zeros((nb, LANES - nb), jnp.float32)], axis=1)
        block = jnp.concatenate([block, jnp.zeros((KP - nb, LANES), jnp.float32)], axis=0)
        gap = jnp.zeros((IM - KP, LANES), jnp.float32)
        block = jnp.concatenate([block, gap, pltpu.roll(block, IM, 1), gap], axis=0)
        block = block.astype(jnp.bfloat16)
        for part, first in ((part_re, 0), (part_im, KP)):
            at = pl.multiple_of((first + a) * pitch, 8)
            inner[pl.ds(at, rows), :] = jnp.dot(
                part, block, preferred_element_type=jnp.float32
            )
        return carry

    load_phi.wait()
    lax.fori_loop(0, nb, contract_b, 0)

    def contract_a(t, carry):
        left = near_mat[pl.ds(t, KP, stride=trip), :]
        left = left[:, 0 : 2 * KP].astype(jnp.bfloat16)
        for quad in range(quads):
            halves = []
            for pair in range(2):
                sides = []
                for one in range(2):
                    m = quad * 4 + pair * 2 + one
                    sides.append(
                        inner[pl.ds(m * trip + t, 2 * KP, stride=pitch), :].astype(
                            jnp.bfloat16
                        )
                    )
                right = jnp.concatenate(sides, axis=1)
                halves.append(jnp.dot(left, right, preferred_element_type=jnp.float32))
            outer[t, quad * 2 * KP : (quad + 1) * 2 * KP, :] = jnp.concatenate(
                halves, axis=0
            ).astype(jnp.bfloat16)
        return carry

    lax.fori_loop(0, trip, contract_a, 0)

    spot = lax.broadcasted_iota(jnp.int32, (sent, sent), 0)
    order = lane_iota((sent, sent)) == spot % n * slots + spot // n
    places[...] = jnp.dot(
        order.astype(jnp.bfloat16), hot_send, preferred_element_type=jnp.float32
    ).astype(jnp.bfloat16)

    at = freq_at - low
    scale = math.sqrt(math.log2(math.e)) / smear_width
    part_freq = pltpu.roll(part_tiles(low // LANES), LANES - at, 1)
    near_freq = pltpu.roll(near_tiles(low // LANES), LANES - at, 1)
    part_freq = jnp.where(lane_iota(part_freq.shape) < nb, part_freq, 1.0)
    part_scaled, part_log = part_freq * scale, -jnp.log2(part_freq)
    first_half = lane_iota((8, LANES)) < IM
    for t in range(trip):
        for pair in range(nb // 2):
            at_row = (t * (nb // 2) + pair) * 8
            for into, of in ((second, part_scaled), (third, part_log)):
                even = jnp.broadcast_to(of[t : t + 1, 2 * pair : 2 * pair + 1], (8, LANES))
                odd = jnp.broadcast_to(
                    of[t : t + 1, 2 * pair + 1 : 2 * pair + 2], (8, LANES)
                )
                into[at_row : at_row + 8, :] = jnp.where(first_half, even, odd)
    near_col = jnp.transpose(
        jnp.concatenate([near_freq, jnp.ones((LANES - trip, LANES), jnp.float32)], axis=0)
    )[0:KP]

    for wave, (near, far) in enumerate(waves):
        count = recvs[wave].shape[0]
        if near == 0:
            recvs[wave][0] = send_ref[me]
            count -= 1
        moved(recvs[wave] if near else send_ref, count, recv_sem.at[wave])
        in_wave = []
        for t in range(trip):
            where = slot_s[t]
            owner = where // slots
            seat_of, here = seat(
                wave,
                lax.rem(owner // 2 - chip + chips, chips),
                lax.rem(owner + core, 2),
            )
            in_wave.append(here)
            pair = recvs[wave][seat_of].astype(jnp.float32)
            row = pair[0:1]
            for s in range(1, slots):
                row = jnp.where(where % slots == s, pair[s : s + 1], row)
            far_rows[t : t + 1, :] = row

        far_tiles = tiles_of(far_rows)
        spread_rows(far_tiles, nb, far_mat, IM, True)
        far_freq = pltpu.roll(far_tiles(low // LANES), LANES - at, 1)
        lanes = lane_iota(far_freq.shape)
        far_freq = jnp.where(lanes < IM, far_freq, pltpu.roll(far_freq, IM, 1))
        used = (lanes % IM) < nb
        far_freq = jnp.where(used, far_freq, 1.0)
        used_cell = (lax.broadcasted_iota(jnp.int32, (KP, LANES), 0) < nb) & (
            lane_iota((KP, LANES)) % IM < nb
        )
        live = live_s[0]

        for t in range(trip):
            ef_re = far_mat[pl.ds(t, KP, stride=trip), :].astype(jnp.bfloat16)
            ef_im = far_mat[pl.ds(KP * trip + t, KP, stride=trip), :].astype(jnp.bfloat16)
            zero = jnp.zeros((IM, LANES), jnp.bfloat16)
            cols = []
            for ef in (ef_re, ef_im):
                ef = jnp.concatenate([ef, zero[0 : IM - KP]], axis=0)
                cols.append(jnp.concatenate([ef, zero], axis=1))
                cols.append(jnp.concatenate([zero, ef], axis=1))
            ef = jnp.concatenate(cols, axis=0)
            w1 = jnp.broadcast_to(near_col[:, t : t + 1], (KP, LANES))
            w3 = jnp.broadcast_to(far_freq[t : t + 1, :], (KP, LANES))
            base = (w1 - w3) * scale
            total = jnp.zeros((KP, LANES), jnp.float32)
            v = lax.dot_general(
                outer[t], ef, (((1,), (1,)), ((), ())), preferred_element_type=jnp.float32
            )
            for pair in range(nb // 2):
                at_row = (t * (nb // 2) + pair) * 8
                w2 = jnp.concatenate([second[at_row : at_row + 8, :]] * (KP // 8), axis=0)
                log = jnp.concatenate([third[at_row : at_row + 8, :]] * (KP // 8), axis=0)
                re = v[pair * KP : (pair + 1) * KP, 0:LANES]
                im = v[pair * KP : (pair + 1) * KP, LANES : 2 * LANES]
                x = base + w2
                total = total + (re * re + im * im) * jnp.exp2(log - x * x)
            keep = used_cell & (in_wave[t] & (t < live))
            total = jnp.where(keep, total / (w1 * w3 * nb), 0.0)
            near_sum = jnp.sum(total, axis=1, keepdims=True)
            near_sum = jnp.broadcast_to(near_sum, (KP, LANES))
            near_acc[t] = near_sum if wave == 0 else near_acc[t] + near_sum
            far_sum = jnp.sum(total, axis=0, keepdims=True)
            far_sum = far_sum + pltpu.roll(far_sum, IM, 1)
            far_acc[t : t + 1, :] = jnp.where(lane_iota(far_sum.shape) < nb, far_sum, 0.0)

        spots = lax.broadcasted_iota(jnp.int32, (n, LANES), 0)
        back = jnp.zeros((n, LANES), jnp.float32)
        for t in range(trip):
            where = slot_s[t]
            row = far_acc[t : t + 1, :]
            for s in range(1, slots):
                row = jnp.where(where % slots == s, pltpu.roll(row, s * LANES // slots, 1), row)
            back = back + jnp.where(spots == where // slots, row, 0.0)
        by_slots[wave][...] = back.reshape(n, 1, LANES)
        if near == 0:
            returned[me] = by_slots[wave][me]
        each(far, near, give_back(wave))
    moved(send_ref, n - 1, send_sem.at[0])

    columns = lane_iota((1, owned))
    rates = jnp.zeros((KP, owned), jnp.float32)
    for t in range(trip):
        spread = jnp.concatenate([near_acc[t]] * (owned // LANES), axis=1)
        rates = rates + jnp.where(columns == local_ref[0:1, t : t + 1], spread, 0.0)

    moved(returned, n - 1, back_send.at[0])
    moved(returned, n - 1, back_recv.at[0])

    filled = returned[...].reshape(n, LANES)
    filled = jnp.concatenate(
        [filled] + [pltpu.roll(filled, LANES - s * LANES // slots, 1) for s in range(1, slots)],
        axis=0,
    )
    filled = jnp.transpose(filled)[0:KP]
    parts = []
    for _ in range(3):
        part = filled.astype(jnp.bfloat16)
        parts.append(part)
        filled = filled - part.astype(jnp.float32)
    placed = jnp.dot(
        jnp.concatenate(parts, axis=0), places[...], preferred_element_type=jnp.float32
    )
    for i in range(3):
        rates = rates + placed[i * KP : (i + 1) * KP]
    out_ref[...] = rates[0:nb]


def on_device(n, eigvec, omega, phi, send_rows, local_q, partner_q, slot_ref, tri_count):
    owned = eigvec.shape[0]
    nb = omega.shape[1]
    trip = local_q.shape[0]
    slots = send_rows.shape[1] // n
    width = -(-(eigvec.shape[1] + nb) // LANES) * LANES
    vmem = pl.BlockSpec(memory_space=pltpu.VMEM)
    hbm = pl.BlockSpec(memory_space=pl.ANY)
    f32 = jnp.float32
    waves = waves_of(n)
    return pl.pallas_call(
        functools.partial(rate_kernel, n, nb, slots),
        out_shape=jax.ShapeDtypeStruct((nb, owned), f32),
        in_specs=[hbm] * 8,
        out_specs=vmem,
        scratch_shapes=[
            pltpu.VMEM((eigvec.shape[1], owned), jnp.bfloat16),
            pltpu.VMEM((nb, owned), jnp.bfloat16),
            pltpu.VMEM(phi.shape, jnp.bfloat16),
            pltpu.VMEM(send_rows.shape, jnp.int32),
            pltpu.VMEM((1, trip), jnp.int32),
            pltpu.VMEM((1, trip), jnp.int32),
            pltpu.SMEM((trip,), jnp.int32),
            pltpu.SMEM((1,), jnp.int32),
            pltpu.VMEM((n, slots, width), jnp.bfloat16),
            pltpu.VMEM((trip, width), f32),
            pltpu.VMEM((trip, width), f32),
            pltpu.VMEM((n * slots, owned), jnp.bfloat16),
            [pltpu.VMEM((wave_rows(n, w), slots, width), jnp.bfloat16) for w in waves],
            pltpu.VMEM((2 * KP * trip, LANES), f32),
            pltpu.VMEM((KP * trip, LANES), f32),
            pltpu.VMEM((2 * KP * trip, LANES), f32),
            pltpu.VMEM((trip, width), f32),
            pltpu.VMEM((2 * KP * (nb * trip + 8), LANES), f32),
            pltpu.VMEM((trip, nb // 2 * KP, 2 * LANES), jnp.bfloat16),
            pltpu.VMEM((trip * nb // 2 * 8, LANES), f32),
            pltpu.VMEM((trip * nb // 2 * 8, LANES), f32),
            pltpu.VMEM((trip, KP, LANES), f32),
            pltpu.VMEM((trip, LANES), f32),
            [pltpu.VMEM((n, 1, LANES), f32) for _ in waves],
            pltpu.VMEM((n, 1, LANES), f32),
            pltpu.SemaphoreType.DMA((1,)),
            pltpu.SemaphoreType.DMA((len(waves),)),
            pltpu.SemaphoreType.DMA((1,)),
            pltpu.SemaphoreType.DMA((1,)),
            pltpu.SemaphoreType.DMA((8,)),
        ],
        compiler_params=pltpu.CompilerParams(
            collective_id=0, has_side_effects=True, vmem_limit_bytes=60 * 1024 * 1024
        ),
    )(
        eigvec.T,
        omega.T,
        phi,
        send_rows,
        local_q.reshape(1, trip),
        partner_q.reshape(1, trip),
        slot_ref,
        tri_count,
    )


def solution(mesh):
    in_specs = (
        P(("groups", "pb"), None),
        P(("groups", "pb"), None),
        P(),
        P(("groups", "pb"), None),
        P(("groups", "pb")),
        P(("groups", "pb")),
        P(("groups", "pb")),
        P(("groups", "pb")),
    )
    out_specs = P(None, ("groups", "pb"))
    return jax.shard_map(
        functools.partial(on_device, mesh.shape["pb"]),
        mesh=mesh,
        in_specs=in_specs,
        out_specs=out_specs,
        check_vma=False,
    )
```

```python
import functools
import math

import jax
import jax.numpy as jnp
from jax import lax
from jax.experimental import pallas as pl
from jax.experimental.pallas import tpu as pltpu
from jax.sharding import PartitionSpec as P

LANES = 128
IM = 64
KP = 40
smear_width = 0.5
MESH = pl.DeviceIdType.MESH


def lane_iota(shape):
    return lax.broadcasted_iota(jnp.int32, shape, len(shape) - 1)


def shifted_window(tiles, start, width, to):
    first, at = divmod(start, LANES)
    moved = pltpu.roll(tiles(first), (to - at) % LANES, 1) if to != at else tiles(first)
    if at + width > LANES:
        after = pltpu.roll(tiles(first + 1), (to - at) % LANES, 1)
        moved = jnp.where(lane_iota(moved.shape) < to + LANES - at, moved, after)
    return moved


def spread_rows(tiles, nb, out_ref, im_at, both):
    half = nb * nb

    def put(k, value):
        count = value.shape[0]
        out_ref[k * count : (k + 1) * count, :] = value

    for k in range(nb):
        re = shifted_window(tiles, k * nb, nb, 0)
        im = shifted_window(tiles, half + k * nb, nb, im_at)
        lanes = lane_iota(re.shape)
        in_re = lanes < nb
        in_im = (lanes >= im_at) & (lanes < im_at + nb)
        put(k, jnp.where(in_re, re, jnp.where(in_im, im, 0.0)))
        if both:
            im0 = shifted_window(tiles, half + k * nb, nb, 0)
            re1 = shifted_window(tiles, k * nb, nb, im_at)
            put(KP + k, jnp.where(in_re, -im0, jnp.where(in_im, re1, 0.0)))
    zero = jnp.zeros(re.shape, jnp.float32)
    for k in range(nb, KP):
        put(k, zero)
        if both:
            put(KP + k, zero)


def picked(index_row, count):
    width = index_row.shape[1]
    hot = lax.broadcasted_iota(jnp.int32, (count, width), 0) == index_row
    return hot.astype(jnp.float32)


def waves_of(n):
    half = n // 4
    cuts = [half // 2 + 1, max(1, 3 * half // 8), max(1, 3 * half // 16), 0]
    waves = zip(cuts, [half] + [cut - 1 for cut in cuts[:-1]])
    return [(near, far) for near, far in waves if near <= far]


def wave_rows(n, wave):
    near, far = wave
    chips = 2 * (far - near + 1) - (near == 0) - (far == n // 4)
    return 2 * chips


def rate_kernel(
    n,
    nb,
    slots,
    eig_hbm,
    omega_hbm,
    phi_hbm,
    rows_hbm,
    local_hbm,
    partner_hbm,
    slot_hbm,
    live_hbm,
    out_ref,
    eig_ref,
    omega_ref,
    phi_ref,
    rows_ref,
    local_ref,
    partner_ref,
    slot_s,
    live_s,
    send_ref,
    near_ref,
    part_ref,
    places,
    recvs,
    mat,
    near_mat,
    far_mat,
    far_rows,
    inner,
    outer,
    second,
    third,
    near_acc,
    far_acc,
    by_slots,
    returned,
    send_sem,
    recv_sem,
    back_send,
    back_recv,
    load_sem,
):
    me = lax.axis_index("pb")
    trip = near_ref.shape[0]
    owned = out_ref.shape[1]
    freq_at = 2 * nb * nb
    quads = nb // 4

    chips = n // 2
    half = chips // 2
    chip, core = me // 2, lax.rem(me, 2)
    waves = waves_of(n)

    def each(far, near, act):
        if far == half:
            act(half, 0)
            act(half, 1)
            far -= 1
        last = max(near, 1)
        if far >= last:

            def step(i, carry):
                d = far - i // 4
                act(jnp.where(i % 4 < 2, d, chips - d), i % 2)
                return carry

            lax.fori_loop(0, 4 * (far - last + 1), step, 0)
        if near == 0:
            act(0, 1)

    def device(r, c):
        return lax.rem(chip + r, chips) * 2 + lax.rem(core + c, 2)

    def seat(wave, r, c):
        near, far = waves[wave]
        first = far - near + 1
        back = chips - min(far, half - 1)
        second = chips - max(near, 1)
        low_side = (r >= near) & (r <= far)
        high_side = (r >= back) & (r <= second)
        row = jnp.where(low_side, r - near, jnp.where(high_side, first + r - back, 0))
        return row * 2 + c, low_side | high_side

    def moved(ref, count, sem):
        every = ref.at[pl.ds(0, count)]
        pltpu.make_async_copy(every, every, sem).wait()

    def exchange(wave):
        def act(r, c):
            to = device(r, c)
            row, _ = seat(wave, lax.rem(chips - r, chips), c)
            pltpu.make_async_remote_copy(
                src_ref=send_ref.at[to],
                dst_ref=recvs[wave].at[row],
                send_sem=send_sem.at[0],
                recv_sem=recv_sem.at[wave],
                device_id={"pb": to},
                device_id_type=MESH,
            ).start()

        return act

    def give_back(wave):
        def act(r, c):
            to = device(r, c)
            pltpu.make_async_remote_copy(
                src_ref=by_slots[wave].at[to],
                dst_ref=returned.at[me],
                send_sem=back_send.at[0],
                recv_sem=back_recv.at[0],
                device_id={"pb": to},
                device_id_type=MESH,
            ).start()

        return act

    load_eig = pltpu.make_async_copy(eig_hbm, eig_ref, load_sem.at[0])
    load_phi = pltpu.make_async_copy(phi_hbm, phi_ref, load_sem.at[1])
    small = (
        (rows_hbm, rows_ref),
        (local_hbm, local_ref),
        (partner_hbm, partner_ref),
        (omega_hbm, omega_ref),
        (slot_hbm, slot_s),
        (live_hbm, live_s),
    )
    loads = [
        pltpu.make_async_copy(source, into, load_sem.at[2 + i])
        for i, (source, into) in enumerate(small)
    ]
    for load in loads + [load_eig, load_phi]:
        load.start()
    barrier = pltpu.get_barrier_semaphore()

    def greet(r, c):
        pl.semaphore_signal(
            barrier, inc=1, device_id={"pb": device(r, c)}, device_id_type=MESH
        )

    each(half, 0, greet)
    for load in loads:
        load.wait()

    rest = jnp.full((1, LANES - 2 * trip), -1, jnp.int32)
    own_row = jnp.concatenate([local_ref[...], partner_ref[...], rest], axis=1)
    hot_send = jnp.transpose(picked(rows_ref[...], owned)).astype(jnp.bfloat16)
    hot_own = jnp.transpose(picked(own_row, owned))[0 : 2 * trip].astype(jnp.bfloat16)
    hot = jnp.concatenate([hot_send, hot_own], axis=0)
    sent = n * slots
    load_eig.wait()
    low = freq_at // LANES * LANES
    tail = jnp.concatenate(
        [
            eig_ref[low:freq_at, :].astype(jnp.float32),
            omega_ref[...].astype(jnp.float32),
            jnp.zeros((low + LANES - freq_at - nb, owned), jnp.float32),
        ],
        axis=0,
    ).astype(jnp.bfloat16)
    piece = 2 * LANES
    for start in range(0, low + LANES, piece):
        end = min(start + piece, low + LANES)
        table = tail if start == low else eig_ref[start:end, :]
        rows = lax.dot_general(
            hot, table, (((1,), (1,)), ((), ())), preferred_element_type=jnp.float32
        )
        send_ref[:, :, start:end] = (
            rows[0:sent].astype(jnp.bfloat16).reshape(n, slots, end - start)
        )
        near_ref[:, start:end] = rows[sent : sent + trip]
        part_ref[:, start:end] = rows[sent + trip : sent + 2 * trip]

    pl.semaphore_wait(barrier, n - 1)

    for wave, (near, far) in enumerate(waves):
        each(far, near, exchange(wave))

    def tiles_of(ref):
        return lambda k: ref[:, k * LANES : (k + 1) * LANES]

    near_tiles, part_tiles = tiles_of(near_ref), tiles_of(part_ref)
    spread_rows(part_tiles, nb, mat, IM, True)
    spread_rows(near_tiles, nb, near_mat, KP, False)

    rows = nb * trip
    pitch = inner.shape[0] // (2 * KP)
    zero_rows = jnp.zeros(((KP - nb) * pitch, LANES), jnp.float32)
    inner[nb * pitch : KP * pitch, :] = zero_rows
    inner[(KP + nb) * pitch : 2 * KP * pitch, :] = zero_rows
    part_re = mat[0:rows, :].astype(jnp.bfloat16)
    part_im = mat[KP * trip : KP * trip + rows, :].astype(jnp.bfloat16)

    def contract_b(a, carry):
        block = phi_ref[a].astype(jnp.float32)
        block = jnp.concatenate([block, jnp.zeros((nb, LANES - nb), jnp.float32)], axis=1)
        block = jnp.concatenate([block, jnp.zeros((KP - nb, LANES), jnp.float32)], axis=0)
        gap = jnp.zeros((IM - KP, LANES), jnp.float32)
        block = jnp.concatenate([block, gap, pltpu.roll(block, IM, 1), gap], axis=0)
        block = block.astype(jnp.bfloat16)
        for part, first in ((part_re, 0), (part_im, KP)):
            at = pl.multiple_of((first + a) * pitch, 8)
            inner[pl.ds(at, rows), :] = jnp.dot(
                part, block, preferred_element_type=jnp.float32
            )
        return carry

    load_phi.wait()
    lax.fori_loop(0, nb, contract_b, 0)

    def contract_a(t, carry):
        left = near_mat[pl.ds(t, KP, stride=trip), :]
        left = left[:, 0 : 2 * KP].astype(jnp.bfloat16)
        for quad in range(quads):
            halves = []
            for pair in range(2):
                sides = []
                for one in range(2):
                    m = quad * 4 + pair * 2 + one
                    sides.append(
                        inner[pl.ds(m * trip + t, 2 * KP, stride=pitch), :].astype(
                            jnp.bfloat16
                        )
                    )
                right = jnp.concatenate(sides, axis=1)
                halves.append(jnp.dot(left, right, preferred_element_type=jnp.float32))
            outer[t, quad * 2 * KP : (quad + 1) * 2 * KP, :] = jnp.concatenate(
                halves, axis=0
            ).astype(jnp.bfloat16)
        return carry

    lax.fori_loop(0, trip, contract_a, 0)

    spot = lax.broadcasted_iota(jnp.int32, (sent, sent), 0)
    order = lane_iota((sent, sent)) == spot % n * slots + spot // n
    places[...] = jnp.dot(
        order.astype(jnp.bfloat16), hot_send, preferred_element_type=jnp.float32
    ).astype(jnp.bfloat16)

    at = freq_at - low
    scale = math.sqrt(math.log2(math.e)) / smear_width
    part_freq = pltpu.roll(part_tiles(low // LANES), LANES - at, 1)
    near_freq = pltpu.roll(near_tiles(low // LANES), LANES - at, 1)
    part_freq = jnp.where(lane_iota(part_freq.shape) < nb, part_freq, 1.0)
    part_scaled, part_log = part_freq * scale, -jnp.log2(part_freq)
    first_half = lane_iota((8, LANES)) < IM
    for t in range(trip):
        for pair in range(nb // 2):
            at_row = (t * (nb // 2) + pair) * 8
            for into, of in ((second, part_scaled), (third, part_log)):
                even = jnp.broadcast_to(of[t : t + 1, 2 * pair : 2 * pair + 1], (8, LANES))
                odd = jnp.broadcast_to(
                    of[t : t + 1, 2 * pair + 1 : 2 * pair + 2], (8, LANES)
                )
                into[at_row : at_row + 8, :] = jnp.where(first_half, even, odd)
    near_col = jnp.transpose(
        jnp.concatenate([near_freq, jnp.ones((LANES - trip, LANES), jnp.float32)], axis=0)
    )[0:KP]

    for wave, (near, far) in enumerate(waves):
        count = recvs[wave].shape[0]
        if near == 0:
            recvs[wave][0] = send_ref[me]
            count -= 1
        moved(recvs[wave] if near else send_ref, count, recv_sem.at[wave])
        in_wave = []
        for t in range(trip):
            where = slot_s[t]
            owner = where // slots
            seat_of, here = seat(
                wave,
                lax.rem(owner // 2 - chip + chips, chips),
                lax.rem(owner + core, 2),
            )
            in_wave.append(here)
            pair = recvs[wave][seat_of].astype(jnp.float32)
            row = pair[0:1]
            for s in range(1, slots):
                row = jnp.where(where % slots == s, pair[s : s + 1], row)
            far_rows[t : t + 1, :] = row

        far_tiles = tiles_of(far_rows)
        spread_rows(far_tiles, nb, far_mat, IM, True)
        far_freq = pltpu.roll(far_tiles(low // LANES), LANES - at, 1)
        lanes = lane_iota(far_freq.shape)
        far_freq = jnp.where(lanes < IM, far_freq, pltpu.roll(far_freq, IM, 1))
        used = (lanes % IM) < nb
        far_freq = jnp.where(used, far_freq, 1.0)
        used_cell = (lax.broadcasted_iota(jnp.int32, (KP, LANES), 0) < nb) & (
            lane_iota((KP, LANES)) % IM < nb
        )
        live = live_s[0]

        for t in range(trip):
            ef_re = far_mat[pl.ds(t, KP, stride=trip), :].astype(jnp.bfloat16)
            ef_im = far_mat[pl.ds(KP * trip + t, KP, stride=trip), :].astype(jnp.bfloat16)
            zero = jnp.zeros((IM, LANES), jnp.bfloat16)
            cols = []
            for ef in (ef_re, ef_im):
                ef = jnp.concatenate([ef, zero[0 : IM - KP]], axis=0)
                cols.append(jnp.concatenate([ef, zero], axis=1))
                cols.append(jnp.concatenate([zero, ef], axis=1))
            ef = jnp.concatenate(cols, axis=0)
            w1 = jnp.broadcast_to(near_col[:, t : t + 1], (KP, LANES))
            w3 = jnp.broadcast_to(far_freq[t : t + 1, :], (KP, LANES))
            base = (w1 - w3) * scale
            total = jnp.zeros((KP, LANES), jnp.float32)
            v = lax.dot_general(
                outer[t], ef, (((1,), (1,)), ((), ())), preferred_element_type=jnp.float32
            )
            for pair in range(nb // 2):
                at_row = (t * (nb // 2) + pair) * 8
                w2 = jnp.concatenate([second[at_row : at_row + 8, :]] * (KP // 8), axis=0)
                log = jnp.concatenate([third[at_row : at_row + 8, :]] * (KP // 8), axis=0)
                re = v[pair * KP : (pair + 1) * KP, 0:LANES]
                im = v[pair * KP : (pair + 1) * KP, LANES : 2 * LANES]
                x = base + w2
                total = total + (re * re + im * im) * jnp.exp2(log - x * x)
            keep = used_cell & (in_wave[t] & (t < live))
            total = jnp.where(keep, total / (w1 * w3 * nb), 0.0)
            near_sum = jnp.sum(total, axis=1, keepdims=True)
            near_sum = jnp.broadcast_to(near_sum, (KP, LANES))
            near_acc[t] = near_sum if wave == 0 else near_acc[t] + near_sum
            far_sum = jnp.sum(total, axis=0, keepdims=True)
            far_sum = far_sum + pltpu.roll(far_sum, IM, 1)
            far_acc[t : t + 1, :] = jnp.where(lane_iota(far_sum.shape) < nb, far_sum, 0.0)

        spots = lax.broadcasted_iota(jnp.int32, (n, LANES), 0)
        back = jnp.zeros((n, LANES), jnp.float32)
        for t in range(trip):
            where = slot_s[t]
            row = far_acc[t : t + 1, :]
            for s in range(1, slots):
                row = jnp.where(where % slots == s, pltpu.roll(row, s * LANES // slots, 1), row)
            back = back + jnp.where(spots == where // slots, row, 0.0)
        by_slots[wave][...] = back.reshape(n, 1, LANES)
        if near == 0:
            returned[me] = by_slots[wave][me]
        each(far, near, give_back(wave))
    moved(send_ref, n - 1, send_sem.at[0])

    columns = lane_iota((1, owned))
    rates = jnp.zeros((KP, owned), jnp.float32)
    for t in range(trip):
        spread = jnp.concatenate([near_acc[t]] * (owned // LANES), axis=1)
        rates = rates + jnp.where(columns == local_ref[0:1, t : t + 1], spread, 0.0)

    moved(returned, n - 1, back_send.at[0])
    moved(returned, n - 1, back_recv.at[0])

    filled = returned[...].reshape(n, LANES)
    filled = jnp.concatenate(
        [filled] + [pltpu.roll(filled, LANES - s * LANES // slots, 1) for s in range(1, slots)],
        axis=0,
    )
    filled = jnp.transpose(filled)[0:KP]
    parts = []
    for _ in range(3):
        part = filled.astype(jnp.bfloat16)
        parts.append(part)
        filled = filled - part.astype(jnp.float32)
    placed = jnp.dot(
        jnp.concatenate(parts, axis=0), places[...], preferred_element_type=jnp.float32
    )
    for i in range(3):
        rates = rates + placed[i * KP : (i + 1) * KP]
    out_ref[...] = rates[0:nb]


def on_device(n, eigvec, omega, phi, send_rows, local_q, partner_q, slot_ref, tri_count):
    owned = eigvec.shape[0]
    nb = omega.shape[1]
    trip = local_q.shape[0]
    slots = send_rows.shape[1] // n
    width = -(-(eigvec.shape[1] + nb) // LANES) * LANES
    vmem = pl.BlockSpec(memory_space=pltpu.VMEM)
    hbm = pl.BlockSpec(memory_space=pl.ANY)
    f32 = jnp.float32
    waves = waves_of(n)
    return pl.pallas_call(
        functools.partial(rate_kernel, n, nb, slots),
        out_shape=jax.ShapeDtypeStruct((nb, owned), f32),
        in_specs=[hbm] * 8,
        out_specs=vmem,
        scratch_shapes=[
            pltpu.VMEM((eigvec.shape[1], owned), jnp.bfloat16),
            pltpu.VMEM((nb, owned), jnp.bfloat16),
            pltpu.VMEM(phi.shape, jnp.bfloat16),
            pltpu.VMEM(send_rows.shape, jnp.int32),
            pltpu.VMEM((1, trip), jnp.int32),
            pltpu.VMEM((1, trip), jnp.int32),
            pltpu.SMEM((trip,), jnp.int32),
            pltpu.SMEM((1,), jnp.int32),
            pltpu.VMEM((n, slots, width), jnp.bfloat16),
            pltpu.VMEM((trip, width), f32),
            pltpu.VMEM((trip, width), f32),
            pltpu.VMEM((n * slots, owned), jnp.bfloat16),
            [pltpu.VMEM((wave_rows(n, w), slots, width), jnp.bfloat16) for w in waves],
            pltpu.VMEM((2 * KP * trip, LANES), f32),
            pltpu.VMEM((KP * trip, LANES), f32),
            pltpu.VMEM((2 * KP * trip, LANES), f32),
            pltpu.VMEM((trip, width), f32),
            pltpu.VMEM((2 * KP * (nb * trip + 8), LANES), f32),
            pltpu.VMEM((trip, nb // 2 * KP, 2 * LANES), jnp.bfloat16),
            pltpu.VMEM((trip * nb // 2 * 8, LANES), f32),
            pltpu.VMEM((trip * nb // 2 * 8, LANES), f32),
            pltpu.VMEM((trip, KP, LANES), f32),
            pltpu.VMEM((trip, LANES), f32),
            [pltpu.VMEM((n, 1, LANES), f32) for _ in waves],
            pltpu.VMEM((n, 1, LANES), f32),
            pltpu.SemaphoreType.DMA((1,)),
            pltpu.SemaphoreType.DMA((len(waves),)),
            pltpu.SemaphoreType.DMA((1,)),
            pltpu.SemaphoreType.DMA((1,)),
            pltpu.SemaphoreType.DMA((8,)),
        ],
        compiler_params=pltpu.CompilerParams(
            collective_id=0, has_side_effects=True, vmem_limit_bytes=60 * 1024 * 1024
        ),
    )(
        eigvec.T,
        omega.T,
        phi,
        send_rows,
        local_q.reshape(1, trip),
        partner_q.reshape(1, trip),
        slot_ref,
        tri_count,
    )


def solution(mesh):
    in_specs = (
        P(("groups", "pb"), None),
        P(("groups", "pb"), None),
        P(),
        P(("groups", "pb"), None),
        P(("groups", "pb")),
        P(("groups", "pb")),
        P(("groups", "pb")),
        P(("groups", "pb")),
    )
    out_specs = P(None, ("groups", "pb"))
    return jax.shard_map(
        functools.partial(on_device, mesh.shape["pb"]),
        mesh=mesh,
        in_specs=in_specs,
        out_specs=out_specs,
        check_vma=False,
    )
```
